128 devices in a mesh: node: 4 (over z), chip: 32 (over x, y, core).
Axes of the slice: x: 4, y: 4, z: 4, core: 2. Of those that a mesh axis runs over, the one named last changes fastest.
Arguments:
- pooled_grad: bfloat16 [8192, 4, 256], P(('node', 'chip')), may hold values from -6 to 6
- grad_scale: bfloat16 [8192, 4], P(('node', 'chip')), may hold values from 0.049804688 to 1
- hot_slot: int32 [8192, 4, 2], P(('node', 'chip')), may hold values from 0 to 511
- send_index: int32 [128, 128, 32], P(('node', 'chip')), may hold values from 0 to 255, as said below
- recv_row: int32 [128, 128, 32], P(('node', 'chip')), may hold values from 0 to 4096, as said below
- cold_weight: float32 [4, 131072, 256], P(None, ('node', 'chip')), may hold values from -3 to 3
- cold_accum: float32 [4, 131072], P(None, ('node', 'chip')), may hold values from 0.5 to 8
- hot_weight: float32 [4, 512, 256], replicated, may hold values from -3 to 3
- hot_accum: float32 [4, 512], replicated, may hold values from 1 to 64
Outputs:
- cold_weight_new: float32 [4, 131072, 256], P(None, ('node', 'chip'))
- cold_accum_new: float32 [4, 131072], P(None, ('node', 'chip'))
- hot_weight_new: float32 [4, 512, 256], replicated
- hot_accum_new: float32 [4, 512], replicated
The draws below stay inside these ranges and needn't reach their ends.
Inputs may be any that keep to these rules, and one draw needn't show every extreme that they name: send_index and recv_row describe the same lookups: slot c from p to q is filled exactly when recv_row[q, p, c] < 4096, the filled slots of a pair come first, and the table in both entries agrees; some owners receive all 32 slots filled from every sender in every draw. `recv_row`: see send_index; empty slots hold 4096.
All inputs are finite; a program needn't handle non-finite values.
Results may differ from the reference program's by a relative error of at most 0.0003.
Values may be sent and summed in bfloat16 or wider, within the bound.
A program may use at most 64 MiB of HBM per device.

```python
import math
import jax
import jax.numpy as jnp
import numpy as np
from jax import lax

D = 256
NT = 4
ROWS_DEV = 1024
B_DEV = 64
LH = 2
HOT = 512
CAP = 32
B = 8192
TABLE_ROWS = 131072
DEVICES = 128


def routing(key):
    keys = jax.random.split(jax.random.fold_in(key, 7), 7)
    order = jax.random.permutation(keys[0], DEVICES)
    heavy = order < max(1, DEVICES // 8)
    filled_count = jax.random.randint(keys[1], (DEVICES, DEVICES), max(1, CAP // 4), CAP // 2 + 1)
    filled_count = jnp.where(heavy[None, :], CAP, filled_count)
    filled = jnp.arange(CAP, dtype=jnp.int32)[None, None, :] < filled_count[:, :, None]
    sample = jax.random.randint(keys[2], (DEVICES, DEVICES, CAP), 0, B_DEV)
    table = jax.random.randint(keys[3], (DEVICES, DEVICES, CAP), 0, NT)
    first = jax.random.randint(keys[4], (DEVICES, DEVICES, CAP), 0, ROWS_DEV)
    second = jax.random.randint(keys[5], (DEVICES, DEVICES, CAP), 0, ROWS_DEV)
    third = jax.random.randint(keys[6], (DEVICES, DEVICES, CAP), 0, ROWS_DEV)
    row = jnp.minimum(jnp.minimum(first, second), third)
    return (filled, sample, table, row)


def draw_send_index(key, part):
    filled, sample, table, row = routing(key)
    return (sample * NT + table).astype(jnp.int32)


def draw_recv_row(key, part):
    filled, sample, table, row = routing(key)
    target = jnp.where(filled, table * ROWS_DEV + row, NT * ROWS_DEV)
    return jnp.transpose(target, (1, 0, 2)).astype(jnp.int32)


def touch_ends(result, stream_key, least, high):
    spot = [jax.random.randint(jax.random.fold_in(stream_key, axis), (), 0, length) for axis, length in enumerate(result.shape)]
    widest = result.shape.index(max(result.shape))
    neighbour = spot[:widest] + [(spot[widest] + 1) % result.shape[widest]] + spot[widest + 1:]
    return result.at[tuple(spot)].set(least).at[tuple(neighbour)].set(high)


def steps_of(stream_key, extent, cuts, low, top_value):
    loudness, own = 1.0, jax.random.fold_in(stream_key, 6)
    for position, shards_of in cuts:
        heights = jnp.exp(jax.random.uniform(jax.random.fold_in(own, position), (shards_of,), jnp.float32, low / len(cuts), top_value / len(cuts)))
        loudness = loudness * jnp.repeat(heights, extent[position] // shards_of).reshape([-1 if axis == position else 1 for axis in range(len(extent))])
    return loudness


def rank_table(amount, lean):
    portions = [(1 << 20) // math.isqrt(standing ** lean) + 1 for standing in range(1, amount + 1)]
    scale = 1 + sum(portions) // (1 << 30)
    return np.cumsum(np.array([max(1, weight // scale) for weight in portions]))


def ranked(stream_key, shape, amount, slope):
    table = rank_table(amount, slope)
    pick = jax.random.randint(jax.random.fold_in(stream_key, 1), shape, 0, int(table[amount - 1]))
    grade = jnp.searchsorted(jnp.asarray(table, jnp.int32), pick, side="right")
    return jax.random.permutation(jax.random.fold_in(stream_key, 2), amount)[grade].astype(jnp.int32)


def noise(own_key, extent, scale, limit, cuts=(), kind=jnp.bfloat16):
    drawn = jax.random.normal(own_key, extent, jnp.float32) * scale
    if len(cuts) > 0:
        drawn = steps_of(own_key, extent, cuts, -0.22, 0.18) * drawn
    return jnp.clip(drawn, min=-limit, max=limit).astype(kind)


def setup_inputs(seed: int = 0) -> dict:
    seeds = jax.random.split(jax.random.key(seed), 10)
    pooled_grad = noise(seeds[0], (B, NT, D), 1.0, 6.0, ((0, 128),))
    grad_scale = jnp.clip(jnp.exp(math.log(1.0) - 2.9996462 * jax.random.uniform(seeds[1], (B, NT), jnp.float32) ** steps_of(seeds[1], (B, NT), ((0, 128),), -0.2, 0.2)), 0.049804688, 1.0).astype(jnp.bfloat16)
    hot_slot = touch_ends(ranked(seeds[2], (B, NT, LH), HOT, 2), jax.random.fold_in(seeds[2], 3), 0, HOT - 1).astype(jnp.int32)
    send_index = draw_send_index(jax.random.fold_in(seeds[9], 71), 0)
    recv_row = draw_recv_row(jax.random.fold_in(seeds[9], 71), 0)
    cold_weight = noise(seeds[5], (NT, TABLE_ROWS, D), 0.5, 3.0, ((1, 128),), jnp.float32)
    cold_accum = jnp.clip(jnp.exp(math.log(8.0) - 2.7725887 * jax.random.uniform(seeds[6], (NT, TABLE_ROWS), jnp.float32) ** steps_of(seeds[6], (NT, TABLE_ROWS), ((1, 128),), -0.2, 0.2)), 0.5, 8.0)
    hot_weight = noise(seeds[7], (NT, HOT, D), 0.5, 3.0, (), jnp.float32)
    hot_accum = jnp.clip(jnp.exp(jax.random.uniform(seeds[8], (NT, HOT), jnp.float32, math.log(1.0), math.log(64.0))), 1.0, 64.0)
    return {"pooled_grad": pooled_grad, "grad_scale": grad_scale, "hot_slot": hot_slot, "send_index": send_index, "recv_row": recv_row, "cold_weight": cold_weight, "cold_accum": cold_accum, "hot_weight": hot_weight, "hot_accum": hot_accum}


LEARN_RATE = 0.5

def adagrad(weight, accum, grad):
    accum_new = accum + lax.optimization_barrier(jnp.mean(grad * grad, axis=-1))
    return (weight - LEARN_RATE * grad / jnp.sqrt(accum_new)[..., None], accum_new)

def reference(pooled_grad, grad_scale, hot_slot, send_index, recv_row, cold_weight, cold_accum, hot_weight, hot_accum):
    dequantized = pooled_grad.astype(jnp.float32) * grad_scale.astype(jnp.float32)[:, :, None]
    grad_rows = dequantized.reshape(B * NT, D)
    local_rows = NT * ROWS_DEV
    senders = jnp.arange(DEVICES, dtype=jnp.int32) * (B_DEV * NT)

    def owner_grad(owner):
        picked = lax.dynamic_index_in_dim(send_index, owner, 1, keepdims=False)
        source = (senders[:, None] + picked.astype(jnp.int32)).reshape(DEVICES * CAP)
        target = lax.dynamic_index_in_dim(recv_row, owner, 0, keepdims=False).reshape(DEVICES * CAP)
        values = jnp.take(grad_rows, source, axis=0)
        return jax.ops.segment_sum(values, target.astype(jnp.int32), num_segments=local_rows + 1)[:local_rows]
    owners = jnp.arange(DEVICES, dtype=jnp.int32)
    cold_grad = lax.map(owner_grad, owners)
    cold_grad = cold_grad.reshape(DEVICES, NT, ROWS_DEV, D).transpose(1, 0, 2, 3).reshape(NT, TABLE_ROWS, D)
    cold_weight_new, cold_accum_new = adagrad(cold_weight, cold_accum, cold_grad)
    table_base = (jnp.arange(NT, dtype=jnp.int32) * HOT)[None, :, None]
    hot_index = (hot_slot.astype(jnp.int32) + table_base).reshape(B * NT * LH)
    spread = jnp.broadcast_to(dequantized[:, :, None, :], (B, NT, LH, D)).reshape(B * NT * LH, D)
    hot_grad = jax.ops.segment_sum(spread, hot_index, num_segments=NT * HOT).reshape(NT, HOT, D)
    hot_weight_new, hot_accum_new = adagrad(hot_weight, hot_accum, hot_grad)
    return (cold_weight_new, cold_accum_new, hot_weight_new, hot_accum_new)
```

```python
import functools
import math

import jax
import jax.numpy as jnp
from jax import lax
from jax.experimental import pallas as pl
from jax.experimental.pallas import tpu as pltpu
from jax.sharding import PartitionSpec as P

NODE_CHIP = ("node", "chip")
MESH = pl.DeviceIdType.MESH
LEARN_RATE = 0.5
SEL = 256
META_ROWS = 48
BLOCK_ROWS = SEL + META_ROWS
ROW_STEP = 512
F32 = jnp.float32
BF16 = jnp.bfloat16


def row_of(tile, row):
    values = tile.astype(F32)
    at = lax.broadcasted_iota(jnp.int32, values.shape, 0) == row
    return jnp.sum(jnp.where(at, values, 0.0), axis=0, keepdims=True)


def exchange_kernel(
    rows, meta, targets, cold_grad, hot_grad,
    g, s, ssc, arrived, scr, hp, hr, hs,
    l0, s1, r1, s2, r2, s3, r3, s4, r4, s5, r5, s6, r6, s7, r7, s8, r8, s9, r9,
):
    z = lax.axis_index("node")
    k = lax.axis_index("chip")
    x, y, c = k // 8, (k // 2) % 4, k % 2
    p1 = y + c * (x - y)
    p2 = x + c * (y - x)
    mine = z * 2 + c
    column = x * 4 + y

    def plane(q1, q2):
        xx = q2 + c * (q1 - q2)
        yy = q1 + c * (q2 - q1)
        return (z, xx * 8 + yy * 2 + c)

    def share(q1, q2):
        xx = q2 + c * (q1 - q2)
        yy = q1 + c * (q2 - q1)
        return xx, yy

    def along_z(m):
        zz, cc = (z + m // 2) % 4, (c + m) % 2
        return zz * 2 + cc, (zz, x * 8 + y * 2 + cc)

    def from_z(m):
        zz, cc = (z + 4 - m // 2) % 4, (c + m) % 2
        return zz * 2 + cc, cc

    local = [
        pltpu.make_async_copy(rows, g.at[p2, p1, pl.ds(0, SEL)], l0.at[0]),
        pltpu.make_async_copy(meta, g.at[p2, p1, pl.ds(SEL, META_ROWS)], l0.at[1]),
    ]
    for copy in local:
        copy.start()

    barrier = pltpu.get_barrier_semaphore()
    for d in (1, 2, 3):
        pl.semaphore_signal(barrier, inc=1, device_id=plane((p1 + d) % 4, p2), device_id_type=MESH)
        pl.semaphore_signal(barrier, inc=1, device_id=plane(p1, (p2 + d) % 4), device_id_type=MESH)
    for m in range(1, 8):
        pl.semaphore_signal(barrier, inc=1, device_id=along_z(m)[1], device_id_type=MESH)
    pl.semaphore_wait(barrier, 13)
    for copy in local:
        copy.wait()

    sends = []

    def send(src, dst, ssem, rsem, dev):
        copy = pltpu.make_async_remote_copy(
            src, dst, ssem, rsem, device_id=dev, device_id_type=MESH
        )
        copy.start()
        sends.append(copy)

    def landed(dst, ssem, rsem):
        pltpu.make_async_remote_copy(
            dst, dst, ssem, rsem, device_id=plane(p1, p2), device_id_type=MESH
        ).wait_recv()

    own = g.at[p2, p1]
    for d in (1, 3, 2):
        send(own, own, s1.at[d], r1.at[d], plane((p1 + d) % 4, p2))
    for d in (1, 3, 2):
        send(own, own, s2.at[d, 0], r2.at[d, 0], plane(p1, (p2 + d) % 4))

    lanes = lax.broadcasted_iota(jnp.int32, (SEL, SEL), 1).astype(F32)
    groups = lax.broadcasted_iota(jnp.int32, (8, SEL), 0)
    owners = lax.broadcasted_iota(jnp.int32, (8, SEL), 1) // 32
    quarter = lax.broadcasted_iota(jnp.int32, (8, 128), 1) // 32
    levels = lax.broadcasted_iota(jnp.int32, (128, SEL), 0).astype(F32)

    def select(b, many):
        picks = [row_of(g[b, a, SEL : SEL + 16, :], column) for a in many]
        pad = [jnp.zeros((8 - len(many), SEL), F32)]
        turned = jnp.transpose(jnp.concatenate(picks + pad, axis=0))
        for n, a in enumerate(many):
            pick = jnp.where(turned[:, n : n + 1] == lanes, 1.0, 0.0).astype(BF16)
            got = jnp.dot(pick, g[b, a, 0:SEL, :], preferred_element_type=F32)
            s[:, b, a] = got.astype(BF16).reshape(8, 32, SEL)
            arrived[mine, b, a] = s[mine, b, a]

    def send_scales(b, chunk):
        total = jnp.zeros((8, 128), F32)
        for a in range(4):
            wide = jnp.where(
                groups == owners, row_of(g[b, a, SEL + 16 : SEL + 32, :], column), 0.0
            )
            half = wide[:, :128] + wide[:, 128:]
            half = half + pltpu.roll(half, 64, 1)
            half = half + pltpu.roll(half, 32, 1)
            total = total + jnp.where(quarter == a, half, 0.0)
        for q in range(8):
            ssc[b, q] = total[q : q + 1]
        scr[mine, b] = ssc[b, mine]
        for m in range(1, 8):
            to, dev = along_z(m)
            send(ssc.at[b, to], scr.at[mine, b], s4.at[m, chunk], r4.at[m, chunk], dev)

    def add_hot(b, first):
        total = jnp.zeros((128, SEL), F32)
        for a in range(4):
            info = g[b, a, SEL + 32 : SEL + 48, :].astype(F32)
            at0 = jnp.where(info[0:1] == column.astype(F32), info[1:2], -1.0)
            at1 = jnp.where(info[2:3] == column.astype(F32), info[3:4], -1.0)
            scale = info[4:5]
            weight = jnp.where(levels == at0, scale, 0.0) + jnp.where(levels == at1, scale, 0.0)
            total = total + jnp.dot(
                weight.astype(BF16), g[b, a, 0:SEL, :], preferred_element_type=F32
            )
        total = total.reshape(8, 16, SEL)
        hp[...] = total if first else hp[...] + total

    def scatter(offset, chunk, first):
        for m in range(1, 8):
            src, cc = from_z(m)
            b = (x + cc * (y - x) + 4 - offset) % 4
            if chunk == 0:
                for j in range(4):
                    a = (y + cc * (x - y) + 4 - j) % 4
                    landed(arrived.at[src, b, a], s3.at[m, j], r3.at[m, j])
            else:
                landed(arrived.at[src, b], s3.at[m, 3 + chunk], r3.at[m, 3 + chunk])
            landed(scr.at[src, b], s4.at[m, chunk], r4.at[m, chunk])
        wanted, scales, values = [], [], []
        for q in range(8):
            cc = q % 2
            b = (x + cc * (y - x) + 4 - offset) % 4
            wanted.append(targets[q, b])
            scales.append(scr[q, b])
            values.append(arrived[q, b].reshape(128, SEL))
        wanted = jnp.concatenate(wanted, axis=1)
        scales = jnp.concatenate(scales, axis=1)
        values = jnp.concatenate(values, axis=0)
        level = lax.broadcasted_iota(jnp.int32, (ROW_STEP, 1024), 0)

        def step(i, carry):
            at = pl.ds(pl.multiple_of(i * ROW_STEP, ROW_STEP), ROW_STEP)
            weight = jnp.where(level == wanted - i * ROW_STEP, scales, 0.0).astype(BF16)
            total = jnp.dot(weight, values, preferred_element_type=F32)
            cold_grad[at, :] = total if first else cold_grad[at, :] + total
            return carry

        lax.fori_loop(0, cold_grad.shape[0] // ROW_STEP, step, 0)

    def send_rows(b, a, slot):
        for m in range(1, 8):
            to, dev = along_z(m)
            if a is None:
                send(s.at[to, b], arrived.at[mine, b], s3.at[m, slot], r3.at[m, slot], dev)
            else:
                send(s.at[to, b, a], arrived.at[mine, b, a], s3.at[m, slot], r3.at[m, slot], dev)

    select(p2, [p1])
    send_rows(p2, p1, 0)
    for j in (1, 3, 2):
        a = (p1 + 4 - j) % 4
        landed(g.at[p2, a], s1.at[j], r1.at[j])
        for d in (1, 3, 2):
            send(g.at[p2, a], g.at[p2, a], s2.at[d, j], r2.at[d, j], plane(p1, (p2 + d) % 4))
        select(p2, [a])
        send_rows(p2, a, j)
    send_scales(p2, 0)
    add_hot(p2, True)

    def next_chunk(n, d):
        b = (p2 + 4 - d) % 4
        for j in (0, 1, 3, 2):
            landed(g.at[b, (p1 + 4 - j) % 4], s2.at[d, j], r2.at[d, j])
        if n == 3:
            add_hot(b, False)
            hr[mine] = hp[mine]
            for m in range(1, 8):
                to, dev = along_z(m)
                send(hp.at[to], hr.at[mine], s5.at[m], r5.at[m], dev)
        select(b, [0, 1, 2, 3])
        send_rows(b, None, 3 + n)
        send_scales(b, n)
        if n < 3:
            add_hot(b, False)

    next_chunk(1, 1)
    next_chunk(2, 3)
    scatter(0, 0, True)
    next_chunk(3, 2)
    scatter(1, 1, False)

    for m in range(1, 8):
        landed(hr.at[from_z(m)[0]], s5.at[m], r5.at[m])
    total = hr[0]
    for q in range(1, 8):
        total = total + hr[q]
    hs[...] = total
    hot_grad[x, y, mine] = total
    for m in range(1, 8):
        send(hs, hot_grad.at[x, y, mine], s6.at[m], r6.at[m], along_z(m)[1])
    scatter(3, 2, False)
    for m in range(1, 8):
        landed(hot_grad.at[x, y, from_z(m)[0]], s6.at[m], r6.at[m])

    part = pl.ds(c * 4, 4)
    twin_part = pl.ds(4 - c * 4, 4)
    twin = along_z(1)[1]
    piece = hot_grad.at[x, y, part]
    for d in (1, 3, 2):
        send(piece, piece, s7.at[d], r7.at[d], plane((p1 + d) % 4, p2))
    for d in (1, 3, 2):
        send(piece, piece, s8.at[d, 0], r8.at[d, 0], plane(p1, (p2 + d) % 4))
    for j in (1, 3, 2):
        xx, yy = share((p1 + 4 - j) % 4, p2)
        piece = hot_grad.at[xx, yy, part]
        landed(piece, s7.at[j], r7.at[j])
        for d in (1, 3, 2):
            send(piece, piece, s8.at[d, j], r8.at[d, j], plane(p1, (p2 + d) % 4))
        send(piece, piece, s9.at[0, j], r9.at[0, j], twin)
    scatter(2, 3, False)
    for d in (1, 3, 2):
        for j in (0, 1, 3, 2):
            xx, yy = share((p1 + 4 - j) % 4, (p2 + 4 - d) % 4)
            piece = hot_grad.at[xx, yy, part]
            landed(piece, s8.at[d, j], r8.at[d, j])
            send(piece, piece, s9.at[d, j], r9.at[d, j], twin)
    for d in range(4):
        for j in range(4):
            if d or j:
                q1 = (x + c * (y - x) + 4 - j) % 4
                q2 = (y + c * (x - y) + 4 - d) % 4
                xx = q1 + c * (q2 - q1)
                yy = q2 + c * (q1 - q2)
                landed(hot_grad.at[xx, yy, twin_part], s9.at[d, j], r9.at[d, j])
    for copy in sends:
        copy.wait_send()


def exchange(rows, meta, targets):
    dma = pltpu.SemaphoreType.DMA
    vmem = pl.BlockSpec(memory_space=pltpu.VMEM)
    hbm = pl.BlockSpec(memory_space=pl.ANY)
    return pl.pallas_call(
        exchange_kernel,
        out_shape=(
            jax.ShapeDtypeStruct((4096, 256), F32),
            jax.ShapeDtypeStruct((4, 4, 8, 16, 256), F32),
        ),
        in_specs=[hbm, hbm, vmem],
        out_specs=(vmem, vmem),
        scratch_shapes=[
            pltpu.VMEM((4, 4, BLOCK_ROWS, 256), BF16),
            pltpu.VMEM((8, 4, 4, 32, 256), BF16),
            pltpu.VMEM((4, 8, 1, 128), F32),
            pltpu.VMEM((8, 4, 4, 32, 256), BF16),
            pltpu.VMEM((8, 4, 1, 128), F32),
            pltpu.VMEM((8, 16, 256), F32),
            pltpu.VMEM((8, 16, 256), F32),
            pltpu.VMEM((16, 256), F32),
            dma((2,)),
            dma((4,)), dma((4,)),
            dma((4, 4)), dma((4, 4)),
            dma((8, 7)), dma((8, 7)),
            dma((8, 4)), dma((8, 4)),
            dma((8,)), dma((8,)),
            dma((8,)), dma((8,)),
            dma((4,)), dma((4,)),
            dma((4, 4)), dma((4, 4)),
            dma((4, 4)), dma((4, 4)),
        ],
        compiler_params=pltpu.CompilerParams(
            collective_id=0, has_side_effects=True, vmem_limit_bytes=48 * 1024 * 1024
        ),
        name="exchange",
    )(rows, meta, targets)


def adagrad_part(grad, weight, accum, weight_new, accum_new):
    eye = lax.broadcasted_iota(jnp.int32, (128, 128), 0) == lax.broadcasted_iota(
        jnp.int32, (128, 128), 1
    )
    for t in range(weight.shape[0]):
        for n in range(weight.shape[1] // 128):
            part = slice(n * 128, n * 128 + 128)
            value = grad[t, part, :]
            mean = jnp.sum(value * value, axis=1, keepdims=True) * (1.0 / value.shape[1])
            old = accum[t : t + 1, part]
            new = jnp.sum(jnp.where(eye, old, 0.0), axis=1, keepdims=True) + mean
            accum_new[t : t + 1, part] = jnp.sum(jnp.where(eye, new, 0.0), axis=0, keepdims=True)
            weight_new[t, part, :] = weight[t, part, :] - value * (LEARN_RATE / jnp.sqrt(new))


def update_kernel(
    cold_grad, cold_weight, cold_accum, hot_grad, hot_weight, hot_accum,
    cold_weight_new, cold_accum_new, hot_weight_new, hot_accum_new,
):
    adagrad_part(cold_grad, cold_weight, cold_accum, cold_weight_new, cold_accum_new)
    adagrad_part(hot_grad, hot_weight, hot_accum, hot_weight_new, hot_accum_new)


def update(cold_grad, cold_weight, cold_accum, hot_grad, hot_weight, hot_accum):
    steps = 4

    def blocks(array):
        shape = list(array.shape)
        shape[1] //= steps
        index = (lambda i: (0, i, 0)) if len(shape) == 3 else (lambda i: (0, i))
        return pl.BlockSpec(tuple(shape), index)

    outs = (cold_weight, cold_accum, hot_weight, hot_accum)
    args = (cold_grad, cold_weight, cold_accum, hot_grad, hot_weight, hot_accum)
    return pl.pallas_call(
        update_kernel,
        grid=(steps,),
        out_shape=tuple(jax.ShapeDtypeStruct(a.shape, F32) for a in outs),
        in_specs=[blocks(a) for a in args],
        out_specs=tuple(blocks(a) for a in outs),
        name="update",
    )(*args)


def meta_of(grad_scale, hot_slot, send_index):
    chosen = send_index.reshape(4, 4, 4, 2, 32).transpose(1, 2, 0, 3, 4).reshape(16, 256)
    sources = jnp.arange(256, dtype=jnp.int32)
    flat_scale = grad_scale.reshape(1, 256)
    out_scale = jnp.sum(
        jnp.where(chosen[:, :, None] == sources, flat_scale.astype(F32), 0.0), axis=-1
    )
    rows = hot_slot + (jnp.arange(4, dtype=jnp.int32) * 512)[None, :, None]
    rows = rows.transpose(2, 0, 1).reshape(2, 256)
    hot = jnp.stack([rows[0] // 128, rows[0] % 128, rows[1] // 128, rows[1] % 128])
    return jnp.concatenate(
        [
            chosen.astype(BF16),
            out_scale.astype(BF16),
            hot.astype(BF16),
            flat_scale,
            jnp.zeros((11, 256), BF16),
        ],
        axis=0,
    )


def per_device(
    pooled_grad,
    grad_scale,
    hot_slot,
    send_index,
    recv_row,
    cold_weight,
    cold_accum,
    hot_weight,
    hot_accum,
):
    width = cold_weight.shape[2]
    rows = pooled_grad.reshape(SEL, width)
    meta = meta_of(grad_scale, hot_slot, send_index)
    received = recv_row.reshape(4, 4, 4, 2, 32)
    targets = jnp.stack(
        [received[:, :, :, 0], received[:, :, :, 1].transpose(0, 2, 1, 3)], axis=1
    ).reshape(8, 4, 1, 128)
    cold_grad, hot_grad = exchange(rows, meta, targets)
    return update(
        cold_grad.reshape(cold_weight.shape),
        cold_weight,
        cold_accum,
        hot_grad.reshape(hot_weight.shape),
        hot_weight,
        hot_accum,
    )


def solution(mesh):
    in_specs = (
        P(NODE_CHIP, None, None),
        P(NODE_CHIP, None),
        P(NODE_CHIP, None, None),
        P(NODE_CHIP, None, None),
        P(NODE_CHIP, None, None),
        P(None, NODE_CHIP, None),
        P(None, NODE_CHIP),
        P(),
        P(),
    )
    out_specs = (P(None, NODE_CHIP, None), P(None, NODE_CHIP), P(), P())
    return jax.shard_map(
        per_device, mesh=mesh, in_specs=in_specs, out_specs=out_specs, check_vma=False
    )
```

```python
import jax
import jax.numpy as jnp
from jax import lax
from jax.experimental import pallas as pl
from jax.experimental.pallas import tpu as pltpu
from jax.sharding import PartitionSpec as P

NODE_CHIP = ("node", "chip")
MESH = pl.DeviceIdType.MESH
LEARN_RATE = 0.5
SEL = 256
BLOCK_ROWS = 288
ROW_STEP = 512
F32 = jnp.float32
BF16 = jnp.bfloat16
FORWARD = (0, 3)
SECOND = (
    (1, 0), (3, 0), (1, 1), (3, 1), (2, 0), (1, 3), (3, 3), (2, 1), (1, 2), (3, 2), (2, 3), (2, 2),
)


def iota(shape, dim):
    return lax.broadcasted_iota(jnp.int32, shape, dim)


def row_of(tile, row):
    values = tile.astype(F32)
    return jnp.sum(jnp.where(iota(values.shape, 0) == row, values, 0.0), axis=0, keepdims=True)


def turned(tile):
    values = tile.astype(F32)
    return jnp.transpose(jnp.concatenate([values, jnp.zeros((96, 128), F32)], axis=0))


def adagrad_rows(value, weight, old):
    eye = iota((128, 128), 0) == iota((128, 128), 1)
    mean = jnp.sum(value * value, axis=1, keepdims=True) * (1.0 / value.shape[1])
    new = jnp.sum(jnp.where(eye, old, 0.0), axis=1, keepdims=True) + mean
    flat = jnp.sum(jnp.where(eye, new, 0.0), axis=0, keepdims=True)
    return weight - value * (LEARN_RATE / jnp.sqrt(new)), flat


def step_kernel(
    rows_in, send_in, scale_in, hot_in, recv_in, cold_weight, cold_accum_in, hot_weight, hot_accum_in,
    cold_new, cold_accum_new, hot_new, hot_accum_new,
    g, s, ssc, arrived, scr, hp, hr, hs, hz, hot_grad, st, tt, cold_w, hot_w,
    rows, send_t, scale_t, hot_t, recv_t, cold_accum, hot_accum, l0, s1, r1, s2, r2, s3, r3, s4, r4, s5, r5, s6, r6, s7, r7, s8, r8, s9, r9,
):
    z = lax.axis_index("node")
    k = lax.axis_index("chip")
    x, y, c = k // 8, (k // 2) % 4, k % 2
    p1 = y + c * (x - y)
    p2 = x + c * (y - x)
    mine = z * 2 + c
    column = x * 4 + y
    part = pl.ds(c * 4, 4)
    twin_part = pl.ds(4 - c * 4, 4)
    twin = (z, x * 8 + y * 2 + 1 - c)

    def plane(q1, q2):
        xx = q2 + c * (q1 - q2)
        yy = q1 + c * (q2 - q1)
        return (z, xx * 8 + yy * 2 + c)

    def share(q1, q2):
        xx = q2 + c * (q1 - q2)
        yy = q1 + c * (q2 - q1)
        return xx, yy

    def along_z(m):
        zz, cc = (z + m // 2) % 4, (c + m) % 2
        return zz * 2 + cc, (zz, x * 8 + y * 2 + cc)

    def from_z(m):
        zz, cc = (z + 4 - m // 2) % 4, (c + m) % 2
        return zz * 2 + cc, cc

    first = [
        pltpu.make_async_copy(src, dst, l0.at[n])
        for n, (src, dst) in enumerate(
            ((rows_in, rows), (send_in, send_t), (scale_in, scale_t), (hot_in, hot_t))
        )
    ]
    later = [
        pltpu.make_async_copy(src, dst, l0.at[4 + n])
        for n, (src, dst) in enumerate(
            (
                (recv_in, recv_t), (cold_accum_in, cold_accum), (hot_accum_in, hot_accum),
                (cold_weight, cold_w), (hot_weight, hot_w),
            )
        )
    ]
    for copy in first:
        copy.start()

    barrier = pltpu.get_barrier_semaphore()
    for d in (1, 2, 3):
        pl.semaphore_signal(barrier, inc=1, device_id=plane((p1 + d) % 4, p2), device_id_type=MESH)
        pl.semaphore_signal(barrier, inc=1, device_id=plane(p1, (p2 + d) % 4), device_id_type=MESH)
    for m in range(1, 8):
        pl.semaphore_signal(barrier, inc=1, device_id=along_z(m)[1], device_id_type=MESH)

    for copy in first:
        copy.wait()
    g[p2, p1, 0:SEL, :] = rows[...].astype(F32).reshape(SEL, SEL).astype(BF16)
    st[...] = turned(send_t[...])
    halves = []
    for half in range(2):
        total = jnp.zeros((16, 128), F32)
        for n in range(4):
            zc = half * 4 + n
            group = st[pl.ds((zc // 2) * 32 + zc % 2, 16, stride=2), :]
            total = total + (pltpu.roll(group, 32 * n, 1) if n else group)
        halves.append(total)
    g[p2, p1, SEL : SEL + 16, :] = jnp.concatenate(halves, axis=1).astype(BF16)
    pieces = []
    for t in range(4):
        slot0, slot1 = hot_t[t, 0:1, :], hot_t[t, 1:2, :]
        pieces.append(
            jnp.concatenate(
                [
                    (slot0 // 128 + t * 4).astype(F32),
                    (slot0 % 128).astype(F32),
                    (slot1 // 128 + t * 4).astype(F32),
                    (slot1 % 128).astype(F32),
                    scale_t[t : t + 1, :].astype(F32),
                    jnp.zeros((3, 64), F32),
                ],
                axis=0,
            )
        )
    info = jnp.concatenate(pieces, axis=1).astype(BF16)
    from_lane = iota((SEL, SEL), 0)
    order = jnp.where((from_lane % 64) * 4 + from_lane // 64 == iota((SEL, SEL), 1), 1.0, 0.0)
    info = jnp.dot(info, order.astype(BF16), preferred_element_type=F32)
    g[p2, p1, SEL + 16 : SEL + 32, :] = jnp.concatenate(
        [info, jnp.zeros((8, SEL), F32)], axis=0
    ).astype(BF16)
    pl.semaphore_wait(barrier, 13)

    sends = []

    def send(src, dst, ssem, rsem, dev):
        copy = pltpu.make_async_remote_copy(
            src, dst, ssem, rsem, device_id=dev, device_id_type=MESH
        )
        copy.start()
        sends.append(copy)

    def landed(dst, ssem, rsem):
        pltpu.make_async_remote_copy(
            dst, dst, ssem, rsem, device_id=plane(p1, p2), device_id_type=MESH
        ).wait_recv()

    own = g.at[p2, p1]
    for d in (1, 3, 2):
        send(own, own, s1.at[d], r1.at[d], plane((p1 + d) % 4, p2))
    for d in (1, 3):
        send(own, own, s2.at[d, 0], r2.at[d, 0], plane(p1, (p2 + d) % 4))
    for copy in later:
        copy.start()

    lanes = iota((SEL, SEL), 1).astype(F32)
    same_owner = iota((8, SEL), 0) == iota((8, SEL), 1) // 32
    quarter = iota((8, 128), 1) // 32
    levels = iota((128, SEL), 0).astype(F32)
    totals = [jnp.zeros((8, 128), F32)] * 4
    hp[...] = jnp.zeros_like(hp)

    def select(b, a, j):
        chosen = row_of(g[b, a, SEL : SEL + 16, :], column)
        chosen = jnp.transpose(jnp.concatenate([chosen, jnp.zeros((7, SEL), F32)], axis=0))
        pick = jnp.where(chosen[:, 0:1] == lanes, 1.0, 0.0).astype(BF16)
        got = jnp.dot(pick, g[b, a, 0:SEL, :], preferred_element_type=F32)
        s[:, b, a] = got.astype(BF16).reshape(8, 32, SEL)
        for m in range(1, 8):
            to, dev = along_z(m)
            slot = j[0] * 4 + j[1]
            send(s.at[to, b, a], arrived.at[mine, b, a], s3.at[m, slot], r3.at[m, slot], dev)
        arrived[mine, b, a] = s[mine, b, a]
        scale = jnp.broadcast_to(g[b, a, SEL + 16 : SEL + 32, :].astype(F32)[4:5], (16, SEL))
        wide = lax.dot_general(
            scale.astype(BF16), pick, (((1,), (1,)), ((), ())), preferred_element_type=F32
        )
        wide = jnp.where(same_owner, wide[0:8], 0.0)
        half = wide[:, :128] + wide[:, 128:]
        half = half + pltpu.roll(half, 64, 1)
        half = half + pltpu.roll(half, 32, 1)
        totals[j[1]] = totals[j[1]] + jnp.where(quarter == b, half, 0.0)

    def send_scales(j):
        a = (p1 + 4 - j) % 4
        for q in range(8):
            ssc[a, q] = totals[j][q : q + 1]
        for m in range(1, 8):
            to, dev = along_z(m)
            send(ssc.at[a, to], scr.at[mine, a], s4.at[m, j], r4.at[m, j], dev)
        scr[mine, a] = ssc[a, mine]

    def add_hot(b, a):
        info = g[b, a, SEL + 16 : SEL + 32, :].astype(F32)
        at0 = jnp.where(info[0:1] == column.astype(F32), info[1:2], -1.0)
        at1 = jnp.where(info[2:3] == column.astype(F32), info[3:4], -1.0)
        scale = info[4:5]
        weight = jnp.where(levels == at0, scale, 0.0) + jnp.where(levels == at1, scale, 0.0)
        total = jnp.dot(weight.astype(BF16), g[b, a, 0:SEL, :], preferred_element_type=F32)
        hp[...] += total.reshape(8, 16, SEL)

    def gathered(q, j):
        zz, cc = q // 2, q % 2
        a = (y + cc * (x - y) + 4 - j) % 4
        wanted = jnp.zeros((1, 128), F32)
        for b in range(4):
            row = tt[pl.ds(zz * 32 + (8 - 6 * cc) * b + (2 + 6 * cc) * a + cc, 1), :]
            wanted = wanted + (pltpu.roll(row, 32 * b, 1) if b else row)
        return wanted, scr[q, a], arrived[q, :, a].reshape(128, SEL)

    def scatter(j, first=False, last=False):
        for m in range(1, 8):
            src, cc = from_z(m)
            a = (y + cc * (x - y) + 4 - j) % 4
            for d in range(4):
                b = (x + cc * (y - x) + 4 - d) % 4
                slot = d * 4 + j
                landed(arrived.at[src, b, a], s3.at[m, slot], r3.at[m, slot])
            landed(scr.at[src, a], s4.at[m, j], r4.at[m, j])
        parts = [gathered(q, j) for q in range(8)]
        wanted = jnp.concatenate([p[0] for p in parts], axis=1)
        scales = jnp.concatenate([p[1] for p in parts], axis=1)
        values = jnp.concatenate([p[2] for p in parts], axis=0)
        level = iota((ROW_STEP, 1024), 0).astype(F32)

        def step(i, carry):
            t, low = i // 2, pl.multiple_of((i % 2) * ROW_STEP, ROW_STEP)
            base = (i * ROW_STEP).astype(F32)
            weight = jnp.where(level == wanted - base, scales, 0.0).astype(BF16)
            total = jnp.dot(weight, values, preferred_element_type=F32)
            if not first:
                total = cold_new[t, pl.ds(low, ROW_STEP), :] + total
            if not last:
                cold_new[t, pl.ds(low, ROW_STEP), :] = total
                return carry
            for n in range(ROW_STEP // 128):
                at = pl.ds(pl.multiple_of(low + n * 128, 128), 128)
                kept = cold_accum_new[:, at]
                fresh, flat = adagrad_rows(
                    total[n * 128 : n * 128 + 128], cold_w[t, at, :], row_of(cold_accum[:, at], t)
                )
                cold_new[t, at, :] = fresh
                cold_accum_new[:, at] = jnp.where(iota((4, 128), 0) == t, flat, kept)
            return carry

        lax.fori_loop(0, 4096 // ROW_STEP, step, 0)

    select(p2, p1, (0, 0))
    add_hot(p2, p1)
    for j in (1, 3, 2):
        a = (p1 + 4 - j) % 4
        landed(g.at[p2, a], s1.at[j], r1.at[j])
        for d in (1, 3):
            send(g.at[p2, a], g.at[p2, a], s2.at[d, j], r2.at[d, j], plane(p1, (p2 + d) % 4))
        select(p2, a, (0, j))
        add_hot(p2, a)

    for d, j in SECOND:
        b, a = (p2 + 4 - d) % 4, (p1 + 4 - j) % 4
        landed(g.at[b, a], s2.at[d, j], r2.at[d, j])
        onward = 1 if j in FORWARD else 3
        if d == onward:
            send(g.at[b, a], g.at[b, a], s2.at[2, j], r2.at[2, j], plane(p1, (p2 + d) % 4))
        add_hot(b, a)
        if (d, j) == SECOND[-1]:
            send(hp.at[twin_part], hr, s5.at[0], r5.at[0], twin)
        select(b, a, (d, j))
        if d == 2:
            send_scales(j)

    for copy in later:
        copy.wait()
    tt[...] = turned(recv_t[...])
    scatter(0, first=True)

    landed(hr, s5.at[0], r5.at[0])
    hs[...] = hp[part] + hr[...]
    for m in (2, 6, 4):
        send(hs, hz.at[m // 2], s6.at[m // 2], r6.at[m // 2], along_z(m)[1])

    scatter(1)

    for m in (1, 3, 2):
        landed(hz.at[m], s6.at[m], r6.at[m])
    hot_grad[x, y, part] = hs[...] + hz[1] + hz[2] + hz[3]
    piece = hot_grad.at[x, y, part]
    for d in (1, 3, 2):
        send(piece, piece, s7.at[d], r7.at[d], plane((p1 + d) % 4, p2))
    for d in (1, 3):
        send(piece, piece, s8.at[d, 0], r8.at[d, 0], plane(p1, (p2 + d) % 4))
    send(piece, piece, s9.at[0, 0], r9.at[0, 0], twin)

    scatter(3)

    for j in (1, 3, 2):
        xx, yy = share((p1 + 4 - j) % 4, p2)
        piece = hot_grad.at[xx, yy, part]
        landed(piece, s7.at[j], r7.at[j])
        for d in (1, 3):
            send(piece, piece, s8.at[d, j], r8.at[d, j], plane(p1, (p2 + d) % 4))
        send(piece, piece, s9.at[0, j], r9.at[0, j], twin)

    def second_piece(d, j):
        xx, yy = share((p1 + 4 - j) % 4, (p2 + 4 - d) % 4)
        piece = hot_grad.at[xx, yy, part]
        landed(piece, s8.at[d, j], r8.at[d, j])
        onward = 1 if j in FORWARD else 3
        if d == onward:
            send(piece, piece, s8.at[2, j], r8.at[2, j], plane(p1, (p2 + d) % 4))
        send(piece, piece, s9.at[d, j], r9.at[d, j], twin)

    second_piece(1, 0)
    second_piece(3, 0)
    scatter(2, last=True)
    for d, j in SECOND[2:]:
        second_piece(d, j)
    for d in range(4):
        for j in range(4):
            q1 = (x + c * (y - x) + 4 - j) % 4
            q2 = (y + c * (x - y) + 4 - d) % 4
            xx = q1 + c * (q2 - q1)
            yy = q2 + c * (q1 - q2)
            landed(hot_grad.at[xx, yy, twin_part], s9.at[d, j], r9.at[d, j])
    for t in range(4):
        for n in range(4):
            at = slice(n * 128, n * 128 + 128)
            fresh, flat = adagrad_rows(
                hot_grad[t, n].reshape(128, SEL), hot_w[t, at, :], hot_accum[t : t + 1, at]
            )
            hot_new[t, at, :] = fresh
            hot_accum_new[t : t + 1, at] = flat
    for copy in sends:
        copy.wait_send()


def step(*args):
    dma = pltpu.SemaphoreType.DMA
    vmem = pl.BlockSpec(memory_space=pltpu.VMEM)
    hbm = pl.BlockSpec(memory_space=pltpu.HBM)
    outs = args[5:]
    args = [pltpu.with_memory_space_constraint(a, pltpu.HBM) for a in args]
    return pl.pallas_call(
        step_kernel,
        out_shape=tuple(jax.ShapeDtypeStruct(a.shape, F32) for a in outs),
        in_specs=[hbm] * 9,
        out_specs=(vmem,) * 4,
        scratch_shapes=[
            pltpu.VMEM((4, 4, BLOCK_ROWS, SEL), BF16),
            pltpu.VMEM((8, 4, 4, 32, SEL), BF16),
            pltpu.VMEM((4, 8, 1, 128), F32),
            pltpu.VMEM((8, 4, 4, 32, SEL), BF16),
            pltpu.VMEM((8, 4, 1, 128), F32),
            pltpu.VMEM((8, 16, SEL), F32),
            pltpu.VMEM((4, 16, SEL), F32),
            pltpu.VMEM((4, 16, SEL), F32),
            pltpu.VMEM((4, 4, 16, SEL), F32),
            pltpu.VMEM((4, 4, 8, 16, SEL), F32),
            pltpu.VMEM((128, 128), F32),
            pltpu.VMEM((128, 128), F32),
            pltpu.VMEM(outs[0].shape, F32),
            pltpu.VMEM(outs[2].shape, F32),
            *(pltpu.VMEM(a.shape, a.dtype) for a in (*args[:5], args[6], args[8])),
            dma((9,)),
            dma((4,)), dma((4,)),
            dma((4, 4)), dma((4, 4)),
            dma((8, 16)), dma((8, 16)),
            dma((8, 4)), dma((8, 4)),
            dma((1,)), dma((1,)),
            dma((4,)), dma((4,)),
            dma((4,)), dma((4,)),
            dma((4, 4)), dma((4, 4)),
            dma((4, 4)), dma((4, 4)),
        ],
        compiler_params=pltpu.CompilerParams(
            collective_id=0, has_side_effects=True, vmem_limit_bytes=40 * 1024 * 1024
        ),
        name="step",
    )(*args)


def per_device(
    pooled_grad,
    grad_scale,
    hot_slot,
    send_index,
    recv_row,
    cold_weight,
    cold_accum,
    hot_weight,
    hot_accum,
):
    return step(
        pooled_grad,
        send_index[0].T,
        grad_scale.T,
        hot_slot.transpose(1, 2, 0),
        recv_row[0].T,
        cold_weight,
        cold_accum,
        hot_weight,
        hot_accum,
    )


def solution(mesh):
    in_specs = (
        P(NODE_CHIP, None, None),
        P(NODE_CHIP, None),
        P(NODE_CHIP, None, None),
        P(NODE_CHIP, None, None),
        P(NODE_CHIP, None, None),
        P(None, NODE_CHIP, None),
        P(None, NODE_CHIP),
        P(),
        P(),
    )
    out_specs = (P(None, NODE_CHIP, None), P(None, NODE_CHIP), P(), P())
    return jax.shard_map(
        per_device, mesh=mesh, in_specs=in_specs, out_specs=out_specs, check_vma=False
    )
```

```python
import jax
import jax.numpy as jnp
from jax import lax
from jax.experimental import pallas as pl
from jax.experimental.pallas import tpu as pltpu
from jax.sharding import PartitionSpec as P

NODE_CHIP = ("node", "chip")
MESH = pl.DeviceIdType.MESH
LEARN_RATE = 0.5
SEL = 256
BLOCK_ROWS = 288
ROW_STEP = 512
F32 = jnp.float32
BF16 = jnp.bfloat16
SECOND = (
    (1, 0), (3, 0), (1, 1), (3, 1), (2, 0), (1, 3), (3, 3), (2, 1), (1, 2), (3, 2), (2, 3), (2, 2),
)
HELD = 6


def iota(shape, dim):
    return lax.broadcasted_iota(jnp.int32, shape, dim)


def row_of(tile, row):
    values = tile.astype(F32)
    return jnp.sum(jnp.where(iota(values.shape, 0) == row, values, 0.0), axis=0, keepdims=True)


def turned(tile):
    values = tile.astype(F32)
    return jnp.transpose(jnp.concatenate([values, jnp.zeros((96, 128), F32)], axis=0))


def columns_of(accum, columns):
    eye = iota((128, 128), 0) == iota((128, 128), 1)
    for t in range(columns.shape[0]):
        for n in range(columns.shape[1] // 128):
            at = slice(n * 128, n * 128 + 128)
            spread = jnp.where(eye, accum[t : t + 1, at], 0.0)
            column = jnp.sum(spread, axis=1, keepdims=True)
            columns[t, at, :] = jnp.broadcast_to(column, (128, 128))


def rows_of(columns, accum):
    eye = iota((128, 128), 0) == iota((128, 128), 1)
    for t in range(columns.shape[0]):
        for n in range(columns.shape[1] // 128):
            at = slice(n * 128, n * 128 + 128)
            row = jnp.sum(jnp.where(eye, columns[t, at, :], 0.0), axis=0, keepdims=True)
            accum[t : t + 1, at] = row


def adagrad_rows(grad, weight, old):
    mean = jnp.sum(grad * grad, axis=1, keepdims=True) * (1.0 / grad.shape[1])
    new = old + mean
    rate = LEARN_RATE / jnp.sqrt(new)
    return weight - grad * jnp.concatenate([rate, rate], axis=1), new


def step_kernel(
    rows_in, send_in, scale_in, hot_in, recv_in, cold_weight, cold_accum_in, hot_weight, hot_accum_in,
    cold_new, cold_accum_new, hot_new, hot_accum_new,
    g, s, ssc, arrived, scr, hp, hr, hs, hz, hot_grad, st, tt, cold_w, hot_w, cold_sum, hot_sum,
    rows, send_t, scale_t, hot_t, recv_t, cold_accum, hot_accum, l0, s1, r1, s2, r2, s3, r3, s4, r4, s5, r5, s6, r6, s7, r7, s8, r8, s9, r9,
):
    z = lax.axis_index("node")
    k = lax.axis_index("chip")
    x, y, c = k // 8, (k // 2) % 4, k % 2
    p1 = y + c * (x - y)
    p2 = x + c * (y - x)
    mine = z * 2 + c
    column = x * 4 + y
    part = pl.ds(c * 4, 4)
    twin_part = pl.ds(4 - c * 4, 4)
    twin = (z, x * 8 + y * 2 + 1 - c)

    def plane(q1, q2):
        xx = q2 + c * (q1 - q2)
        yy = q1 + c * (q2 - q1)
        return (z, xx * 8 + yy * 2 + c)

    def share(q1, q2):
        xx = q2 + c * (q1 - q2)
        yy = q1 + c * (q2 - q1)
        return xx, yy

    def along_z(m):
        zz, cc = (z + m // 2) % 4, (c + m) % 2
        return zz * 2 + cc, (zz, x * 8 + y * 2 + cc)

    def from_z(m):
        zz, cc = (z + 4 - m // 2) % 4, (c + m) % 2
        return zz * 2 + cc, cc

    first = [
        pltpu.make_async_copy(src, dst, l0.at[n])
        for n, (src, dst) in enumerate(
            ((rows_in, rows), (send_in, send_t), (scale_in, scale_t), (hot_in, hot_t))
        )
    ]
    later = [
        pltpu.make_async_copy(src, dst, l0.at[4 + n])
        for n, (src, dst) in enumerate(
            (
                (recv_in, recv_t), (cold_accum_in, cold_accum), (hot_accum_in, hot_accum),
                (cold_weight, cold_w), (hot_weight, hot_w),
            )
        )
    ]
    for copy in first:
        copy.start()

    barrier = pltpu.get_barrier_semaphore()
    for d in (1, 2, 3):
        pl.semaphore_signal(barrier, inc=1, device_id=plane((p1 + d) % 4, p2), device_id_type=MESH)
        pl.semaphore_signal(barrier, inc=1, device_id=plane(p1, (p2 + d) % 4), device_id_type=MESH)
    for m in range(1, 8):
        pl.semaphore_signal(barrier, inc=1, device_id=along_z(m)[1], device_id_type=MESH)

    for copy in first:
        copy.wait()
    g[p2, p1, 0:SEL, :] = rows[...].astype(F32).reshape(SEL, SEL).astype(BF16)
    st[...] = turned(send_t[...])
    halves = []
    for half in range(2):
        total = jnp.zeros((16, 128), F32)
        for n in range(4):
            zc = half * 4 + n
            group = st[pl.ds((zc // 2) * 32 + zc % 2, 16, stride=2), :]
            total = total + (pltpu.roll(group, 32 * n, 1) if n else group)
        halves.append(total)
    g[p2, p1, SEL : SEL + 16, :] = jnp.concatenate(halves, axis=1).astype(BF16)
    pieces = []
    for t in range(4):
        slot0, slot1 = hot_t[t, 0:1, :], hot_t[t, 1:2, :]
        pieces.append(
            jnp.concatenate(
                [
                    (slot0 // 128 + t * 4).astype(F32),
                    (slot0 % 128).astype(F32),
                    (slot1 // 128 + t * 4).astype(F32),
                    (slot1 % 128).astype(F32),
                    scale_t[t : t + 1, :].astype(F32),
                    jnp.zeros((3, 64), F32),
                ],
                axis=0,
            )
        )
    info = jnp.concatenate(pieces, axis=1).astype(BF16)
    from_lane = iota((SEL, SEL), 0)
    order = jnp.where((from_lane % 64) * 4 + from_lane // 64 == iota((SEL, SEL), 1), 1.0, 0.0)
    info = jnp.dot(info, order.astype(BF16), preferred_element_type=F32)
    g[p2, p1, SEL + 16 : SEL + 32, :] = jnp.concatenate(
        [info, jnp.zeros((8, SEL), F32)], axis=0
    ).astype(BF16)
    pl.semaphore_wait(barrier, 13)

    sends = []

    def send(src, dst, ssem, rsem, dev):
        copy = pltpu.make_async_remote_copy(
            src, dst, ssem, rsem, device_id=dev, device_id_type=MESH
        )
        copy.start()
        sends.append(copy)

    def landed(dst, ssem, rsem):
        pltpu.make_async_remote_copy(
            dst, dst, ssem, rsem, device_id=plane(p1, p2), device_id_type=MESH
        ).wait_recv()

    own = g.at[p2, p1]
    for d in (1, 3, 2):
        send(own, own, s1.at[d], r1.at[d], plane((p1 + d) % 4, p2))
    for d in (1, 3, 2):
        send(own, own, s2.at[d, 0], r2.at[d, 0], plane(p1, (p2 + d) % 4))
    for copy in later:
        copy.start()

    lanes = iota((SEL, SEL), 1).astype(F32)
    same_owner = iota((8, SEL), 0) == iota((8, SEL), 1) // 32
    quarter = iota((8, 128), 1) // 32
    levels = iota((128, SEL), 0).astype(F32)
    totals = [jnp.zeros((8, 128), F32)] * 4
    hp[...] = jnp.zeros_like(hp)

    def select(b, a, j):
        chosen = row_of(g[b, a, SEL : SEL + 16, :], column)
        chosen = jnp.transpose(jnp.concatenate([chosen, jnp.zeros((7, SEL), F32)], axis=0))
        pick = jnp.where(chosen[:, 0:1] == lanes, 1.0, 0.0).astype(BF16)
        got = jnp.dot(pick, g[b, a, 0:SEL, :], preferred_element_type=F32)
        s[:, b, a] = got.astype(BF16).reshape(8, 32, SEL)
        for m in range(1, 8):
            to, dev = along_z(m)
            slot = j[0] * 4 + j[1]
            send(s.at[to, b, a], arrived.at[mine, b, a], s3.at[m, slot], r3.at[m, slot], dev)
        arrived[mine, b, a] = s[mine, b, a]
        scale = jnp.broadcast_to(g[b, a, SEL + 16 : SEL + 32, :].astype(F32)[4:5], (16, SEL))
        wide = lax.dot_general(
            scale.astype(BF16), pick, (((1,), (1,)), ((), ())), preferred_element_type=F32
        )
        wide = jnp.where(same_owner, wide[0:8], 0.0)
        half = wide[:, :128] + wide[:, 128:]
        half = half + pltpu.roll(half, 64, 1)
        half = half + pltpu.roll(half, 32, 1)
        totals[j[1]] = totals[j[1]] + jnp.where(quarter == b, half, 0.0)

    def send_scales(j):
        a = (p1 + 4 - j) % 4
        for q in range(8):
            ssc[a, q] = totals[j][q : q + 1]
        for m in range(1, 8):
            to, dev = along_z(m)
            send(ssc.at[a, to], scr.at[mine, a], s4.at[m, j], r4.at[m, j], dev)
        scr[mine, a] = ssc[a, mine]

    def add_hot(b, a):
        info = g[b, a, SEL + 16 : SEL + 32, :].astype(F32)
        at0 = jnp.where(info[0:1] == column.astype(F32), info[1:2], -1.0)
        at1 = jnp.where(info[2:3] == column.astype(F32), info[3:4], -1.0)
        scale = info[4:5]
        weight = jnp.where(levels == at0, scale, 0.0) + jnp.where(levels == at1, scale, 0.0)
        total = jnp.dot(weight.astype(BF16), g[b, a, 0:SEL, :], preferred_element_type=F32)
        hp[...] += total.reshape(8, 16, SEL)

    def gathered(q, j):
        zz, cc = q // 2, q % 2
        a = (y + cc * (x - y) + 4 - j) % 4
        wanted = jnp.zeros((1, 128), F32)
        for b in range(4):
            row = tt[pl.ds(zz * 32 + (8 - 6 * cc) * b + (2 + 6 * cc) * a + cc, 1), :]
            wanted = wanted + (pltpu.roll(row, 32 * b, 1) if b else row)
        return wanted, scr[q, a], arrived[q, :, a].reshape(128, SEL)

    def chunk(j):
        for m in range(1, 8):
            src, cc = from_z(m)
            a = (y + cc * (x - y) + 4 - j) % 4
            for d in range(4):
                b = (x + cc * (y - x) + 4 - d) % 4
                slot = d * 4 + j
                landed(arrived.at[src, b, a], s3.at[m, slot], r3.at[m, slot])
            landed(scr.at[src, a], s4.at[m, j], r4.at[m, j])
        parts = [gathered(q, j) for q in range(8)]
        wanted = jnp.concatenate([p[0] for p in parts], axis=1)
        scales = jnp.concatenate([p[1] for p in parts], axis=1)
        values = jnp.concatenate([p[2] for p in parts], axis=0)
        return wanted, scales, values

    def scatter(parts, low_step, high_step, first=False, last=False):
        wanted, scales, values = parts
        level = iota((ROW_STEP, 1024), 0).astype(F32)

        def step(i, carry):
            t, low = i // 2, pl.multiple_of((i % 2) * ROW_STEP, ROW_STEP)
            base = (i * ROW_STEP).astype(F32)
            weight = jnp.where(level == wanted - base, scales, 0.0).astype(BF16)
            total = jnp.dot(weight, values, preferred_element_type=F32)
            if not first:
                total = cold_new[t, pl.ds(low, ROW_STEP), :] + total
            if not last:
                cold_new[t, pl.ds(low, ROW_STEP), :] = total
                return carry
            at = pl.ds(low, ROW_STEP)
            fresh, new = adagrad_rows(total, cold_w[t, at, :], cold_sum[t, at, :])
            cold_new[t, at, :] = fresh
            cold_sum[t, at, :] = new
            return carry

        lax.fori_loop(low_step, high_step, step, 0)

    select(p2, p1, (0, 0))
    add_hot(p2, p1)
    for copy in later:
        copy.wait()
    tt[...] = turned(recv_t[...])
    columns_of(cold_accum, cold_sum)
    columns_of(hot_accum, hot_sum)
    for j in (1, 3, 2):
        a = (p1 + 4 - j) % 4
        landed(g.at[p2, a], s1.at[j], r1.at[j])
        for d in (1, 3, 2):
            send(g.at[p2, a], g.at[p2, a], s2.at[d, j], r2.at[d, j], plane(p1, (p2 + d) % 4))
        select(p2, a, (0, j))
        add_hot(p2, a)

    def pass_on(d, j):
        select((p2 + 4 - d) % 4, (p1 + 4 - j) % 4, (d, j))
        if d == 2:
            send_scales(j)

    for n, (d, j) in enumerate(SECOND):
        b, a = (p2 + 4 - d) % 4, (p1 + 4 - j) % 4
        landed(g.at[b, a], s2.at[d, j], r2.at[d, j])
        add_hot(b, a)
        if n < len(SECOND) - HELD:
            pass_on(d, j)
    send(hp.at[twin_part], hr, s5.at[0], r5.at[0], twin)
    for d, j in SECOND[-HELD : 2 - HELD]:
        pass_on(d, j)
    landed(hr, s5.at[0], r5.at[0])
    hs[...] = hp[part] + hr[...]
    for m in (2, 6, 4):
        send(hs, hz.at[m // 2], s6.at[m // 2], r6.at[m // 2], along_z(m)[1])
    for d, j in SECOND[2 - HELD :]:
        pass_on(d, j)

    steps = 4096 // ROW_STEP
    scatter(chunk(0), 0, steps, first=True)
    for m in (1, 3, 2):
        landed(hz.at[m], s6.at[m], r6.at[m])
    hot_grad[x, y, part] = hs[...] + hz[1] + hz[2] + hz[3]
    piece = hot_grad.at[x, y, part]
    for d in (1, 3, 2):
        send(piece, piece, s7.at[d], r7.at[d], plane((p1 + d) % 4, p2))
    for d in (1, 3, 2):
        send(piece, piece, s8.at[d, 0], r8.at[d, 0], plane(p1, (p2 + d) % 4))
    send(piece, piece, s9.at[0, 0], r9.at[0, 0], twin)
    scatter(chunk(1), 0, steps)
    for j in (1, 3, 2):
        xx, yy = share((p1 + 4 - j) % 4, p2)
        piece = hot_grad.at[xx, yy, part]
        landed(piece, s7.at[j], r7.at[j])
        for d in (1, 3, 2):
            send(piece, piece, s8.at[d, j], r8.at[d, j], plane(p1, (p2 + d) % 4))
        send(piece, piece, s9.at[0, j], r9.at[0, j], twin)
    scatter(chunk(3), 0, steps)
    scatter(chunk(2), 0, steps, last=True)
    rows_of(cold_sum, cold_accum_new)
    for j in (0, 1, 3, 2):
        for d in (1, 3, 2):
            xx, yy = share((p1 + 4 - j) % 4, (p2 + 4 - d) % 4)
            piece = hot_grad.at[xx, yy, part]
            landed(piece, s8.at[d, j], r8.at[d, j])
            send(piece, piece, s9.at[d, j], r9.at[d, j], twin)
    for j in (0, 1, 3, 2):
        for d in (0, 1, 3, 2):
            q1 = (x + c * (y - x) + 4 - j) % 4
            q2 = (y + c * (x - y) + 4 - d) % 4
            xx = q1 + c * (q2 - q1)
            yy = q2 + c * (q1 - q2)
            landed(hot_grad.at[xx, yy, twin_part], s9.at[d, j], r9.at[d, j])
    for t in range(4):
        fresh, new = adagrad_rows(hot_grad[t].reshape(512, SEL), hot_w[t], hot_sum[t])
        hot_new[t] = fresh
        hot_sum[t] = new
    rows_of(hot_sum, hot_accum_new)
    for copy in sends:
        copy.wait_send()


def step(*args):
    dma = pltpu.SemaphoreType.DMA
    vmem = pl.BlockSpec(memory_space=pltpu.VMEM)
    hbm = pl.BlockSpec(memory_space=pltpu.HBM)
    outs = args[5:]
    args = [pltpu.with_memory_space_constraint(a, pltpu.HBM) for a in args]
    return pl.pallas_call(
        step_kernel,
        out_shape=tuple(jax.ShapeDtypeStruct(a.shape, F32) for a in outs),
        in_specs=[hbm] * 9,
        out_specs=(vmem,) * 4,
        scratch_shapes=[
            pltpu.VMEM((4, 4, BLOCK_ROWS, SEL), BF16),
            pltpu.VMEM((8, 4, 4, 32, SEL), BF16),
            pltpu.VMEM((4, 8, 1, 128), F32),
            pltpu.VMEM((8, 4, 4, 32, SEL), BF16),
            pltpu.VMEM((8, 4, 1, 128), F32),
            pltpu.VMEM((8, 16, SEL), F32),
            pltpu.VMEM((4, 16, SEL), F32),
            pltpu.VMEM((4, 16, SEL), F32),
            pltpu.VMEM((4, 4, 16, SEL), F32),
            pltpu.VMEM((4, 4, 8, 16, SEL), F32),
            pltpu.VMEM((128, 128), F32),
            pltpu.VMEM((128, 128), F32),
            pltpu.VMEM(outs[0].shape, F32),
            pltpu.VMEM(outs[2].shape, F32),
            pltpu.VMEM((*outs[0].shape[:2], 128), F32),
            pltpu.VMEM((*outs[2].shape[:2], 128), F32),
            *(pltpu.VMEM(a.shape, a.dtype) for a in (*args[:5], args[6], args[8])),
            dma((9,)),
            dma((4,)), dma((4,)),
            dma((4, 4)), dma((4, 4)),
            dma((8, 16)), dma((8, 16)),
            dma((8, 4)), dma((8, 4)),
            dma((1,)), dma((1,)),
            dma((4,)), dma((4,)),
            dma((4,)), dma((4,)),
            dma((4, 4)), dma((4, 4)),
            dma((4, 4)), dma((4, 4)),
        ],
        compiler_params=pltpu.CompilerParams(
            collective_id=0, has_side_effects=True, vmem_limit_bytes=40 * 1024 * 1024
        ),
        name="step",
    )(*args)


def leave_kernel(*refs):
    sem = refs[-1]
    copies = [
        pltpu.make_async_copy(refs[n], refs[4 + n], sem.at[n]) for n in range(4)
    ]
    for copy in copies:
        copy.start()
    for copy in copies:
        copy.wait()


def leave(*arrays):
    return pl.pallas_call(
        leave_kernel,
        out_shape=tuple(jax.ShapeDtypeStruct(a.shape, a.dtype) for a in arrays),
        in_specs=[pl.BlockSpec(memory_space=pltpu.VMEM)] * 4,
        out_specs=(pl.BlockSpec(memory_space=pl.ANY),) * 4,
        scratch_shapes=[pltpu.SemaphoreType.DMA((4,))],
        compiler_params=pltpu.CompilerParams(vmem_limit_bytes=16 * 1024 * 1024),
        name="leave",
    )(*arrays)


def per_device(
    pooled_grad,
    grad_scale,
    hot_slot,
    send_index,
    recv_row,
    cold_weight,
    cold_accum,
    hot_weight,
    hot_accum,
):
    results = step(
        pooled_grad,
        send_index[0].T,
        grad_scale.T,
        hot_slot.transpose(1, 2, 0),
        recv_row[0].T,
        cold_weight,
        cold_accum,
        hot_weight,
        hot_accum,
    )
    return leave(*results)


def solution(mesh):
    in_specs = (
        P(NODE_CHIP, None, None),
        P(NODE_CHIP, None),
        P(NODE_CHIP, None, None),
        P(NODE_CHIP, None, None),
        P(NODE_CHIP, None, None),
        P(None, NODE_CHIP, None),
        P(None, NODE_CHIP),
        P(),
        P(),
    )
    out_specs = (P(None, NODE_CHIP, None), P(None, NODE_CHIP), P(), P())
    return jax.shard_map(
        per_device, mesh=mesh, in_specs=in_specs, out_specs=out_specs, check_vma=False
    )
```

```python
import jax
import jax.numpy as jnp
from jax import lax
from jax.experimental import pallas as pl
from jax.experimental.pallas import tpu as pltpu
from jax.sharding import PartitionSpec as P

NODE_CHIP = ("node", "chip")
MESH = pl.DeviceIdType.MESH
LEARN_RATE = 0.5
SEL = 256
BLOCK_ROWS = 288
ROW_STEP = 512
F32 = jnp.float32
BF16 = jnp.bfloat16


def iota(shape, dim):
    return lax.broadcasted_iota(jnp.int32, shape, dim)


def row_of(tile, row):
    values = tile.astype(F32)
    return jnp.sum(jnp.where(iota(values.shape, 0) == row, values, 0.0), axis=0, keepdims=True)


def turned(tile):
    values = tile.astype(F32)
    return jnp.transpose(jnp.concatenate([values, jnp.zeros((96, 128), F32)], axis=0))


def columns_of(accum, columns):
    eye = iota((128, 128), 0) == iota((128, 128), 1)
    for t in range(columns.shape[0]):
        for n in range(columns.shape[1] // 128):
            at = slice(n * 128, n * 128 + 128)
            spread = jnp.where(eye, accum[t : t + 1, at], 0.0)
            column = jnp.sum(spread, axis=1, keepdims=True)
            columns[t, at, :] = jnp.broadcast_to(column, (128, 128))


def rows_of(columns, accum):
    eye = iota((128, 128), 0) == iota((128, 128), 1)
    for t in range(columns.shape[0]):
        for n in range(columns.shape[1] // 128):
            at = slice(n * 128, n * 128 + 128)
            row = jnp.sum(jnp.where(eye, columns[t, at, :], 0.0), axis=0, keepdims=True)
            accum[t : t + 1, at] = row


def adagrad_rows(grad, weight, old):
    mean = jnp.sum(grad * grad, axis=1, keepdims=True) * (1.0 / grad.shape[1])
    new = old + mean
    rate = LEARN_RATE / jnp.sqrt(new)
    return weight - grad * jnp.concatenate([rate, rate], axis=1), new


def step_kernel(
    rows_in, send_in, scale_in, hot_in, recv_in, cold_weight, cold_accum_in, hot_weight, hot_accum_in,
    cold_new, cold_accum_new, hot_new, hot_accum_new,
    g, s, ssc, arrived, scr, hp, hr, hs, hz, hot_grad, st, tt, cold_w, hot_w, cold_sum, hot_sum,
    rows, send_t, scale_t, hot_t, recv_t, cold_accum, hot_accum, l0, s1, r1, s2, r2, s3, r3, s4, r4, s5, r5, s6, r6, s7, r7, s8, r8, s9, r9, sa, ra,
):
    z = lax.axis_index("node")
    k = lax.axis_index("chip")
    x, y, c = k // 8, (k // 2) % 4, k % 2
    p1 = y + c * (x - y)
    p2 = x + c * (y - x)
    mine = z * 2 + c
    column = x * 4 + y
    part = pl.ds(c * 4, 4)
    twin_part = pl.ds(4 - c * 4, 4)
    twin = (z, x * 8 + y * 2 + 1 - c)

    def plane(q1, q2):
        xx = q2 + c * (q1 - q2)
        yy = q1 + c * (q2 - q1)
        return (z, xx * 8 + yy * 2 + c)

    def share(q1, q2):
        xx = q2 + c * (q1 - q2)
        yy = q1 + c * (q2 - q1)
        return xx, yy

    def along_z(m):
        zz, cc = (z + m // 2) % 4, (c + m) % 2
        return zz * 2 + cc, (zz, x * 8 + y * 2 + cc)

    def from_z(m):
        zz, cc = (z + 4 - m // 2) % 4, (c + m) % 2
        return zz * 2 + cc, cc

    first = [
        pltpu.make_async_copy(src, dst, l0.at[n])
        for n, (src, dst) in enumerate(
            ((rows_in, rows), (send_in, send_t), (scale_in, scale_t), (hot_in, hot_t))
        )
    ]
    later = [
        pltpu.make_async_copy(src, dst, l0.at[4 + n])
        for n, (src, dst) in enumerate(
            (
                (recv_in, recv_t), (cold_accum_in, cold_accum), (hot_accum_in, hot_accum),
                (cold_weight, cold_w), (hot_weight, hot_w),
            )
        )
    ]
    for copy in first:
        copy.start()

    barrier = pltpu.get_barrier_semaphore()
    for d in (1, 2, 3):
        pl.semaphore_signal(barrier, inc=1, device_id=plane((p1 + d) % 4, p2), device_id_type=MESH)
        pl.semaphore_signal(barrier, inc=1, device_id=plane(p1, (p2 + d) % 4), device_id_type=MESH)
    for m in range(1, 8):
        pl.semaphore_signal(barrier, inc=1, device_id=along_z(m)[1], device_id_type=MESH)

    for copy in first:
        copy.wait()
    by_sample = rows[...].astype(F32)
    for t in range(4):
        g[p2, p1, t * 64 : t * 64 + 64, :] = by_sample[:, t, :].astype(BF16)
    picks = send_t[...]
    st[...] = turned((picks % 4) * 64 + picks // 4)
    halves = []
    for half in range(2):
        total = jnp.zeros((16, 128), F32)
        for n in range(4):
            zc = half * 4 + n
            group = st[pl.ds((zc // 2) * 32 + zc % 2, 16, stride=2), :]
            total = total + (pltpu.roll(group, 32 * n, 1) if n else group)
        halves.append(total)
    g[p2, p1, SEL : SEL + 16, :] = jnp.concatenate(halves, axis=1).astype(BF16)
    pieces = []
    for t in range(4):
        slot0, slot1 = hot_t[t, 0:1, :], hot_t[t, 1:2, :]
        pieces.append(
            jnp.concatenate(
                [
                    (slot0 // 128 + t * 4).astype(F32),
                    (slot0 % 128).astype(F32),
                    (slot1 // 128 + t * 4).astype(F32),
                    (slot1 % 128).astype(F32),
                    scale_t[t : t + 1, :].astype(F32),
                    jnp.zeros((3, 64), F32),
                ],
                axis=0,
            )
        )
    info = jnp.concatenate(pieces, axis=1)
    g[p2, p1, SEL + 16 : SEL + 32, :] = jnp.concatenate(
        [info, jnp.zeros((8, SEL), F32)], axis=0
    ).astype(BF16)
    pl.semaphore_wait(barrier, 13)

    sends = []

    def send(src, dst, ssem, rsem, dev):
        copy = pltpu.make_async_remote_copy(
            src, dst, ssem, rsem, device_id=dev, device_id_type=MESH
        )
        copy.start()
        sends.append(copy)

    def landed(dst, ssem, rsem):
        pltpu.make_async_remote_copy(
            dst, dst, ssem, rsem, device_id=plane(p1, p2), device_id_type=MESH
        ).wait_recv()

    own = g.at[p2, p1]
    for d in (1, 3, 2):
        send(own, own, s1.at[d], r1.at[d], plane((p1 + d) % 4, p2))
    for d in (1, 3, 2):
        send(own, own, s2.at[d, 0], r2.at[d, 0], plane(p1, (p2 + d) % 4))
    for copy in later:
        copy.start()

    lanes = iota((SEL, SEL), 1).astype(F32)
    same_owner = iota((8, SEL), 0) == iota((8, SEL), 1) // 32
    quarter = iota((8, 128), 1) // 32
    levels = iota((128, 64), 0).astype(F32)
    table = pl.ds(pl.multiple_of(x * 64, 64), 64)
    totals = [jnp.zeros((8, 128), F32)] * 4
    hp[...] = jnp.zeros_like(hp)

    def select(b, a, j):
        chosen = row_of(g[b, a, SEL : SEL + 16, :], column)
        chosen = jnp.transpose(jnp.concatenate([chosen, jnp.zeros((7, SEL), F32)], axis=0))
        pick = jnp.where(chosen[:, 0:1] == lanes, 1.0, 0.0).astype(BF16)
        got = jnp.dot(pick, g[b, a, 0:SEL, :], preferred_element_type=F32)
        s[:, b, a] = got.astype(BF16).reshape(8, 32, SEL)
        for m in range(1, 8):
            to, dev = along_z(m)
            slot = j[0] * 4 + j[1]
            send(s.at[to, b, a], arrived.at[mine, b, a], s3.at[m, slot], r3.at[m, slot], dev)
        arrived[mine, b, a] = s[mine, b, a]
        scale = jnp.broadcast_to(g[b, a, SEL + 16 : SEL + 32, :].astype(F32)[4:5], (16, SEL))
        wide = lax.dot_general(
            scale.astype(BF16), pick, (((1,), (1,)), ((), ())), preferred_element_type=F32
        )
        wide = jnp.where(same_owner, wide[0:8], 0.0)
        half = wide[:, :128] + wide[:, 128:]
        half = half + pltpu.roll(half, 64, 1)
        half = half + pltpu.roll(half, 32, 1)
        totals[j[1]] = totals[j[1]] + jnp.where(quarter == b, half, 0.0)

    def send_scales(j):
        a = (p1 + 4 - j) % 4
        for q in range(8):
            ssc[a, q] = totals[j][q : q + 1]
        for m in range(1, 8):
            to, dev = along_z(m)
            send(ssc.at[a, to], scr.at[mine, a], s4.at[m, j], r4.at[m, j], dev)
        scr[mine, a] = ssc[a, mine]

    def add_hot(b, a):
        info = pltpu.roll(g[b, a, SEL + 16 : SEL + 32, :].astype(F32), (SEL - x * 64) % SEL, 1)
        info = info[:, 0:64]
        at0 = jnp.where(info[0:1] == column.astype(F32), info[1:2], -1.0)
        at1 = jnp.where(info[2:3] == column.astype(F32), info[3:4], -1.0)
        scale = info[4:5]
        weight = jnp.where(levels == at0, scale, 0.0) + jnp.where(levels == at1, scale, 0.0)
        total = jnp.dot(weight.astype(BF16), g[b, a, table, :], preferred_element_type=F32)
        hp[...] += total.reshape(8, 16, SEL)

    def gathered(q, j):
        zz, cc = q // 2, q % 2
        a = (y + cc * (x - y) + 4 - j) % 4
        wanted = jnp.zeros((1, 128), F32)
        for b in range(4):
            row = tt[pl.ds(zz * 32 + (8 - 6 * cc) * b + (2 + 6 * cc) * a + cc, 1), :]
            wanted = wanted + (pltpu.roll(row, 32 * b, 1) if b else row)
        return wanted, scr[q, a], arrived[q, :, a].reshape(128, SEL)

    def chunk(j):
        for m in range(1, 8):
            src, cc = from_z(m)
            a = (y + cc * (x - y) + 4 - j) % 4
            for d in range(4):
                b = (x + cc * (y - x) + 4 - d) % 4
                slot = d * 4 + j
                landed(arrived.at[src, b, a], s3.at[m, slot], r3.at[m, slot])
            landed(scr.at[src, a], s4.at[m, j], r4.at[m, j])
        parts = [gathered(q, j) for q in range(8)]
        wanted = jnp.concatenate([p[0] for p in parts], axis=1)
        scales = jnp.concatenate([p[1] for p in parts], axis=1)
        values = jnp.concatenate([p[2] for p in parts], axis=0)
        return wanted, scales, values

    def scatter(parts, low_step, high_step, first=False, last=False):
        wanted, scales, values = parts
        level = iota((ROW_STEP, 1024), 0).astype(F32)

        def step(i, carry):
            t, low = i // 2, pl.multiple_of((i % 2) * ROW_STEP, ROW_STEP)
            base = (i * ROW_STEP).astype(F32)
            weight = jnp.where(level == wanted - base, scales, 0.0).astype(BF16)
            total = jnp.dot(weight, values, preferred_element_type=F32)
            if not first:
                total = cold_new[t, pl.ds(low, ROW_STEP), :] + total
            if not last:
                cold_new[t, pl.ds(low, ROW_STEP), :] = total
                return carry
            at = pl.ds(low, ROW_STEP)
            fresh, new = adagrad_rows(total, cold_w[t, at, :], cold_sum[t, at, :])
            cold_new[t, at, :] = fresh
            cold_sum[t, at, :] = new
            return carry

        lax.fori_loop(low_step, high_step, step, 0)

    def piece_of(b, a, n, xx):
        if n == 4:
            return g.at[b, a, pl.ds(SEL, 32)]
        return g.at[b, a, pl.ds(pl.multiple_of(((xx + n) % 4) * 64, 64), 64)]

    def forward(d, j, parts):
        a = (p1 + 4 - j) % 4
        far = share(p1, (p2 + d) % 4)[0]
        for n in parts:
            ref = piece_of(p2, a, n, far)
            send(ref, ref, sa.at[d, j, n], ra.at[d, j, n], plane(p1, (p2 + d) % 4))

    def arrives(d, j, parts):
        for n in parts:
            landed(
                piece_of((p2 + 4 - d) % 4, (p1 + 4 - j) % 4, n, x), sa.at[d, j, n], ra.at[d, j, n]
            )

    select(p2, p1, (0, 0))
    add_hot(p2, p1)
    for copy in later:
        copy.wait()
    tt[...] = turned(recv_t[...])
    columns_of(cold_accum, cold_sum)
    columns_of(hot_accum, hot_sum)
    for j in (1, 3, 2):
        a = (p1 + 4 - j) % 4
        landed(g.at[p2, a], s1.at[j], r1.at[j])
        for d in (1, 3, 2):
            forward(d, j, (0, 4))
        select(p2, a, (0, j))
        add_hot(p2, a)

    def pass_on(d, j):
        select((p2 + 4 - d) % 4, (p1 + 4 - j) % 4, (d, j))
        if d == 2:
            send_scales(j)

    for j in (1, 3, 2):
        for d in (1, 3, 2):
            forward(d, j, (1, 2, 3))
    for d in (1, 3, 2):
        b = (p2 + 4 - d) % 4
        landed(g.at[b, p1], s2.at[d, 0], r2.at[d, 0])
        add_hot(b, p1)
        pass_on(d, 0)
    for j in (1, 3, 2):
        for d in (1, 3, 2):
            arrives(d, j, (0, 4))
            add_hot((p2 + 4 - d) % 4, (p1 + 4 - j) % 4)
    send(hp.at[twin_part], hr, s5.at[0], r5.at[0], twin)
    landed(hr, s5.at[0], r5.at[0])
    hs[...] = hp[part] + hr[...]
    for m in (2, 6, 4):
        send(hs, hz.at[m // 2], s6.at[m // 2], r6.at[m // 2], along_z(m)[1])
    for j in (1, 3, 2):
        for d in (1, 3, 2):
            arrives(d, j, (1, 2, 3))
            pass_on(d, j)

    for m in (1, 3, 2):
        landed(hz.at[m], s6.at[m], r6.at[m])
    hot_grad[x, y, part] = hs[...] + hz[1] + hz[2] + hz[3]
    piece = hot_grad.at[x, y, part]
    for d in (1, 3, 2):
        send(piece, piece, s7.at[d], r7.at[d], plane((p1 + d) % 4, p2))
    for d in (1, 3, 2):
        send(piece, piece, s8.at[d, 0], r8.at[d, 0], plane(p1, (p2 + d) % 4))
    send(piece, piece, s9.at[0, 0], r9.at[0, 0], twin)
    steps = 4096 // ROW_STEP
    scatter(chunk(0), 0, steps, first=True)
    for j in (1, 3, 2):
        xx, yy = share((p1 + 4 - j) % 4, p2)
        piece = hot_grad.at[xx, yy, part]
        landed(piece, s7.at[j], r7.at[j])
        for d in (1, 3, 2):
            send(piece, piece, s8.at[d, j], r8.at[d, j], plane(p1, (p2 + d) % 4))
        send(piece, piece, s9.at[0, j], r9.at[0, j], twin)
    scatter(chunk(1), 0, steps)
    scatter(chunk(3), 0, steps)
    for j in (0, 1, 3, 2):
        for d in (1, 3, 2):
            xx, yy = share((p1 + 4 - j) % 4, (p2 + 4 - d) % 4)
            piece = hot_grad.at[xx, yy, part]
            landed(piece, s8.at[d, j], r8.at[d, j])
            send(piece, piece, s9.at[d, j], r9.at[d, j], twin)
    scatter(chunk(2), 0, steps, last=True)
    rows_of(cold_sum, cold_accum_new)
    for j in (0, 1, 3, 2):
        for d in (0, 1, 3, 2):
            q1 = (x + c * (y - x) + 4 - j) % 4
            q2 = (y + c * (x - y) + 4 - d) % 4
            xx = q1 + c * (q2 - q1)
            yy = q2 + c * (q1 - q2)
            landed(hot_grad.at[xx, yy, twin_part], s9.at[d, j], r9.at[d, j])
    for t in range(4):
        fresh, new = adagrad_rows(hot_grad[t].reshape(512, SEL), hot_w[t], hot_sum[t])
        hot_new[t] = fresh
        hot_sum[t] = new
    rows_of(hot_sum, hot_accum_new)
    for copy in sends:
        copy.wait_send()


def step(*args):
    dma = pltpu.SemaphoreType.DMA
    vmem = pl.BlockSpec(memory_space=pltpu.VMEM)
    hbm = pl.BlockSpec(memory_space=pltpu.HBM)
    outs = args[5:]
    args = [pltpu.with_memory_space_constraint(a, pltpu.HBM) for a in args]
    return pl.pallas_call(
        step_kernel,
        out_shape=tuple(jax.ShapeDtypeStruct(a.shape, F32) for a in outs),
        in_specs=[hbm] * 9,
        out_specs=(vmem,) * 4,
        scratch_shapes=[
            pltpu.VMEM((4, 4, BLOCK_ROWS, SEL), BF16),
            pltpu.VMEM((8, 4, 4, 32, SEL), BF16),
            pltpu.VMEM((4, 8, 1, 128), F32),
            pltpu.VMEM((8, 4, 4, 32, SEL), BF16),
            pltpu.VMEM((8, 4, 1, 128), F32),
            pltpu.VMEM((8, 16, SEL), F32),
            pltpu.VMEM((4, 16, SEL), F32),
            pltpu.VMEM((4, 16, SEL), F32),
            pltpu.VMEM((4, 4, 16, SEL), F32),
            pltpu.VMEM((4, 4, 8, 16, SEL), F32),
            pltpu.VMEM((128, 128), F32),
            pltpu.VMEM((128, 128), F32),
            pltpu.VMEM(outs[0].shape, F32),
            pltpu.VMEM(outs[2].shape, F32),
            pltpu.VMEM((*outs[0].shape[:2], 128), F32),
            pltpu.VMEM((*outs[2].shape[:2], 128), F32),
            *(pltpu.VMEM(a.shape, a.dtype) for a in (*args[:5], args[6], args[8])),
            dma((9,)),
            dma((4,)), dma((4,)),
            dma((4, 4)), dma((4, 4)),
            dma((8, 16)), dma((8, 16)),
            dma((8, 4)), dma((8, 4)),
            dma((1,)), dma((1,)),
            dma((4,)), dma((4,)),
            dma((4,)), dma((4,)),
            dma((4, 4)), dma((4, 4)),
            dma((4, 4)), dma((4, 4)),
            dma((4, 4, 5)), dma((4, 4, 5)),
        ],
        compiler_params=pltpu.CompilerParams(
            collective_id=0, has_side_effects=True, vmem_limit_bytes=40 * 1024 * 1024
        ),
        name="step",
    )(*args)


def leave_kernel(*refs):
    sem = refs[-1]
    copies = [
        pltpu.make_async_copy(refs[n], refs[4 + n], sem.at[n]) for n in range(4)
    ]
    for copy in copies:
        copy.start()
    for copy in copies:
        copy.wait()


def leave(*arrays):
    return pl.pallas_call(
        leave_kernel,
        out_shape=tuple(jax.ShapeDtypeStruct(a.shape, a.dtype) for a in arrays),
        in_specs=[pl.BlockSpec(memory_space=pltpu.VMEM)] * 4,
        out_specs=(pl.BlockSpec(memory_space=pl.ANY),) * 4,
        scratch_shapes=[pltpu.SemaphoreType.DMA((4,))],
        compiler_params=pltpu.CompilerParams(vmem_limit_bytes=16 * 1024 * 1024),
        name="leave",
    )(*arrays)


def per_device(
    pooled_grad,
    grad_scale,
    hot_slot,
    send_index,
    recv_row,
    cold_weight,
    cold_accum,
    hot_weight,
    hot_accum,
):
    results = step(
        pooled_grad,
        send_index[0].T,
        grad_scale.T,
        hot_slot.transpose(1, 2, 0),
        recv_row[0].T,
        cold_weight,
        cold_accum,
        hot_weight,
        hot_accum,
    )
    return leave(*results)


def solution(mesh):
    in_specs = (
        P(NODE_CHIP, None, None),
        P(NODE_CHIP, None),
        P(NODE_CHIP, None, None),
        P(NODE_CHIP, None, None),
        P(NODE_CHIP, None, None),
        P(None, NODE_CHIP, None),
        P(None, NODE_CHIP),
        P(),
        P(),
    )
    out_specs = (P(None, NODE_CHIP, None), P(None, NODE_CHIP), P(), P())
    return jax.shard_map(
        per_device, mesh=mesh, in_specs=in_specs, out_specs=out_specs, check_vma=False
    )
```

```python
import jax
import jax.numpy as jnp
from jax import lax
from jax.experimental import pallas as pl
from jax.experimental.pallas import tpu as pltpu
from jax.sharding import PartitionSpec as P

NODE_CHIP = ("node", "chip")
MESH = pl.DeviceIdType.MESH
LEARN_RATE = 0.5
SEL = 256
BLOCK_ROWS = 288
ROW_STEP = 1024
PER_TABLE = 1024 // ROW_STEP
F32 = jnp.float32
BF16 = jnp.bfloat16


def iota(shape, dim):
    return lax.broadcasted_iota(jnp.int32, shape, dim)


def row_of(tile, row):
    values = tile.astype(F32)
    return jnp.sum(jnp.where(iota(values.shape, 0) == row, values, 0.0), axis=0, keepdims=True)


def turned(tile):
    values = tile.astype(F32)
    return jnp.transpose(jnp.concatenate([values, jnp.zeros((96, 128), F32)], axis=0))


def columns_of(accum, columns):
    eye = iota((128, 128), 0) == iota((128, 128), 1)
    for t in range(columns.shape[0]):
        for n in range(columns.shape[1] // 128):
            at = slice(n * 128, n * 128 + 128)
            spread = jnp.where(eye, accum[t : t + 1, at], 0.0)
            column = jnp.sum(spread, axis=1, keepdims=True)
            columns[t, at, :] = jnp.broadcast_to(column, (128, 128))


def rows_of(columns, accum):
    eye = iota((128, 128), 0) == iota((128, 128), 1)
    for t in range(columns.shape[0]):
        for n in range(columns.shape[1] // 128):
            at = slice(n * 128, n * 128 + 128)
            row = jnp.sum(jnp.where(eye, columns[t, at, :], 0.0), axis=0, keepdims=True)
            accum[t : t + 1, at] = row


def adagrad_rows(grad, weight, old):
    mean = jnp.sum(grad * grad, axis=1, keepdims=True) * (1.0 / grad.shape[1])
    new = old + mean
    rate = LEARN_RATE / jnp.sqrt(new)
    return weight - grad * jnp.concatenate([rate, rate], axis=1), new


def step_kernel(
    rows_in, send_in, scale_in, hot_in, recv_in, cold_weight, cold_accum_in, hot_weight, hot_accum_in,
    cold_new, cold_accum_new, hot_new, hot_accum_new,
    g, s, ssc, arrived, scr, hp, hr, hs, hz, hot_grad, st, tt, cold_w, hot_w, cold_sum, hot_sum,
    rows, send_t, scale_t, hot_t, recv_t, cold_accum, hot_accum, l0, s1, r1, s2, r2, s3, r3, s4, r4, s5, r5, s6, r6, s7, r7, s8, r8, s9, r9, sa, ra,
):
    z = lax.axis_index("node")
    k = lax.axis_index("chip")
    x, y, c = k // 8, (k // 2) % 4, k % 2
    p1 = y + c * (x - y)
    p2 = x + c * (y - x)
    mine = z * 2 + c
    column = x * 4 + y
    part = pl.ds(c * 4, 4)
    twin_part = pl.ds(4 - c * 4, 4)
    twin = (z, x * 8 + y * 2 + 1 - c)

    def plane(q1, q2):
        xx = q2 + c * (q1 - q2)
        yy = q1 + c * (q2 - q1)
        return (z, xx * 8 + yy * 2 + c)

    def share(q1, q2):
        xx = q2 + c * (q1 - q2)
        yy = q1 + c * (q2 - q1)
        return xx, yy

    def along_z(m):
        zz, cc = (z + m // 2) % 4, (c + m) % 2
        return zz * 2 + cc, (zz, x * 8 + y * 2 + cc)

    def from_z(m):
        zz, cc = (z + 4 - m // 2) % 4, (c + m) % 2
        return zz * 2 + cc, cc

    first = [
        pltpu.make_async_copy(src, dst, l0.at[n])
        for n, (src, dst) in enumerate(
            ((rows_in, rows), (send_in, send_t), (scale_in, scale_t), (hot_in, hot_t))
        )
    ]
    later = [
        pltpu.make_async_copy(src, dst, l0.at[4 + n])
        for n, (src, dst) in enumerate(
            (
                (recv_in, recv_t), (cold_accum_in, cold_accum), (hot_accum_in, hot_accum),
                (cold_weight, cold_w), (hot_weight, hot_w),
            )
        )
    ]
    for copy in first:
        copy.start()

    barrier = pltpu.get_barrier_semaphore()
    for d in (1, 2, 3):
        pl.semaphore_signal(barrier, inc=1, device_id=plane((p1 + d) % 4, p2), device_id_type=MESH)
        pl.semaphore_signal(barrier, inc=1, device_id=plane(p1, (p2 + d) % 4), device_id_type=MESH)
    for m in range(1, 8):
        pl.semaphore_signal(barrier, inc=1, device_id=along_z(m)[1], device_id_type=MESH)

    for copy in first:
        copy.wait()
    by_sample = rows[...].astype(F32)
    for t in range(4):
        g[p2, p1, t * 64 : t * 64 + 64, :] = by_sample[:, t, :].astype(BF16)
    picks = send_t[...]
    st[...] = turned((picks % 4) * 64 + picks // 4)
    halves = []
    for half in range(2):
        total = jnp.zeros((16, 128), F32)
        for n in range(4):
            zc = half * 4 + n
            group = st[pl.ds((zc // 2) * 32 + zc % 2, 16, stride=2), :]
            total = total + (pltpu.roll(group, 32 * n, 1) if n else group)
        halves.append(total)
    g[p2, p1, SEL : SEL + 16, :] = jnp.concatenate(halves, axis=1).astype(BF16)
    pieces = []
    for t in range(4):
        slot0, slot1 = hot_t[t, 0:1, :], hot_t[t, 1:2, :]
        pieces.append(
            jnp.concatenate(
                [
                    (slot0 // 128 + t * 4).astype(F32),
                    (slot0 % 128).astype(F32),
                    (slot1 // 128 + t * 4).astype(F32),
                    (slot1 % 128).astype(F32),
                    scale_t[t : t + 1, :].astype(F32),
                    jnp.zeros((3, 64), F32),
                ],
                axis=0,
            )
        )
    info = jnp.concatenate(pieces, axis=1)
    g[p2, p1, SEL + 16 : SEL + 32, :] = jnp.concatenate(
        [info, jnp.zeros((8, SEL), F32)], axis=0
    ).astype(BF16)
    pl.semaphore_wait(barrier, 13)

    sends = []

    def send(src, dst, ssem, rsem, dev):
        copy = pltpu.make_async_remote_copy(
            src, dst, ssem, rsem, device_id=dev, device_id_type=MESH
        )
        copy.start()
        sends.append(copy)

    def landed(dst, ssem, rsem):
        pltpu.make_async_remote_copy(
            dst, dst, ssem, rsem, device_id=plane(p1, p2), device_id_type=MESH
        ).wait_recv()

    own = g.at[p2, p1]
    for d in (1, 3, 2):
        send(own, own, s1.at[d], r1.at[d], plane((p1 + d) % 4, p2))
    for d in (1, 3, 2):
        send(own, own, s2.at[d, 0], r2.at[d, 0], plane(p1, (p2 + d) % 4))
    for copy in later:
        copy.start()

    lanes = iota((SEL, SEL), 1).astype(F32)
    same_owner = iota((8, SEL), 0) == iota((8, SEL), 1) // 32
    quarter = iota((8, 128), 1) // 32
    levels = iota((128, 64), 0).astype(F32)
    table = pl.ds(pl.multiple_of(x * 64, 64), 64)
    totals = [jnp.zeros((8, 128), F32)] * 4
    hp[...] = jnp.zeros_like(hp)

    def select(b, a, j):
        chosen = row_of(g[b, a, SEL : SEL + 16, :], column)
        chosen = jnp.transpose(jnp.concatenate([chosen, jnp.zeros((7, SEL), F32)], axis=0))
        pick = jnp.where(chosen[:, 0:1] == lanes, 1.0, 0.0).astype(BF16)
        got = jnp.dot(pick, g[b, a, 0:SEL, :], preferred_element_type=F32)
        s[:, b, a] = got.astype(BF16).reshape(8, 32, SEL)
        for m in range(1, 8):
            to, dev = along_z(m)
            slot = j[0] * 4 + j[1]
            send(s.at[to, b, a], arrived.at[mine, b, a], s3.at[m, slot], r3.at[m, slot], dev)
        arrived[mine, b, a] = s[mine, b, a]
        scale = jnp.broadcast_to(g[b, a, SEL + 16 : SEL + 32, :].astype(F32)[4:5], (16, SEL))
        wide = lax.dot_general(
            scale.astype(BF16), pick, (((1,), (1,)), ((), ())), preferred_element_type=F32
        )
        wide = jnp.where(same_owner, wide[0:8], 0.0)
        half = wide[:, :128] + wide[:, 128:]
        half = half + pltpu.roll(half, 64, 1)
        half = half + pltpu.roll(half, 32, 1)
        totals[j[1]] = totals[j[1]] + jnp.where(quarter == b, half, 0.0)

    def send_scales(j):
        a = (p1 + 4 - j) % 4
        for q in range(8):
            ssc[a, q] = totals[j][q : q + 1]
        for m in range(1, 8):
            to, dev = along_z(m)
            send(ssc.at[a, to], scr.at[mine, a], s4.at[m, j], r4.at[m, j], dev)
        scr[mine, a] = ssc[a, mine]

    def add_hot(b, a):
        info = pltpu.roll(g[b, a, SEL + 16 : SEL + 32, :].astype(F32), (SEL - x * 64) % SEL, 1)
        info = info[:, 0:64]
        at0 = jnp.where(info[0:1] == column.astype(F32), info[1:2], -1.0)
        at1 = jnp.where(info[2:3] == column.astype(F32), info[3:4], -1.0)
        scale = info[4:5]
        weight = jnp.where(levels == at0, scale, 0.0) + jnp.where(levels == at1, scale, 0.0)
        total = jnp.dot(weight.astype(BF16), g[b, a, table, :], preferred_element_type=F32)
        hp[...] += total.reshape(8, 16, SEL)

    def gathered(q, j):
        zz, cc = q // 2, q % 2
        a = (y + cc * (x - y) + 4 - j) % 4
        wanted = jnp.zeros((1, 128), F32)
        for b in range(4):
            row = tt[pl.ds(zz * 32 + (8 - 6 * cc) * b + (2 + 6 * cc) * a + cc, 1), :]
            wanted = wanted + (pltpu.roll(row, 32 * b, 1) if b else row)
        return wanted, scr[q, a], arrived[q, :, a].reshape(128, SEL)

    def chunk(j):
        for m in range(1, 8):
            src, cc = from_z(m)
            a = (y + cc * (x - y) + 4 - j) % 4
            for d in range(4):
                b = (x + cc * (y - x) + 4 - d) % 4
                slot = d * 4 + j
                landed(arrived.at[src, b, a], s3.at[m, slot], r3.at[m, slot])
            landed(scr.at[src, a], s4.at[m, j], r4.at[m, j])
        parts = [gathered(q, j) for q in range(8)]
        wanted = jnp.concatenate([p[0] for p in parts], axis=1)
        scales = jnp.concatenate([p[1] for p in parts], axis=1)
        values = jnp.concatenate([p[2] for p in parts], axis=0)
        return wanted, scales, values

    def scatter(parts, low_step, high_step, first=False, last=False):
        wanted, scales, values = parts
        level = iota((ROW_STEP, 1024), 0).astype(F32)

        def step(i, carry):
            t, low = i // PER_TABLE, pl.multiple_of((i % PER_TABLE) * ROW_STEP, ROW_STEP)
            base = (i * ROW_STEP).astype(F32)
            weight = jnp.where(level == wanted - base, scales, 0.0).astype(BF16)
            total = jnp.dot(weight, values, preferred_element_type=F32)
            if not first:
                total = cold_new[t, pl.ds(low, ROW_STEP), :] + total
            if not last:
                cold_new[t, pl.ds(low, ROW_STEP), :] = total
                return carry
            at = pl.ds(low, ROW_STEP)
            fresh, new = adagrad_rows(total, cold_w[t, at, :], cold_sum[t, at, :])
            cold_new[t, at, :] = fresh
            cold_sum[t, at, :] = new
            return carry

        lax.fori_loop(low_step, high_step, step, 0)

    def piece_of(b, a, n, xx):
        if n == 4:
            return g.at[b, a, pl.ds(SEL, 32)]
        return g.at[b, a, pl.ds(pl.multiple_of(((xx + n) % 4) * 64, 64), 64)]

    def forward(d, j, parts):
        a = (p1 + 4 - j) % 4
        far = share(p1, (p2 + d) % 4)[0]
        for n in parts:
            ref = piece_of(p2, a, n, far)
            send(ref, ref, sa.at[d, j, n], ra.at[d, j, n], plane(p1, (p2 + d) % 4))

    def arrives(d, j, parts):
        for n in parts:
            landed(
                piece_of((p2 + 4 - d) % 4, (p1 + 4 - j) % 4, n, x), sa.at[d, j, n], ra.at[d, j, n]
            )

    select(p2, p1, (0, 0))
    add_hot(p2, p1)
    for copy in later:
        copy.wait()
    tt[...] = turned(recv_t[...])
    columns_of(cold_accum, cold_sum)
    columns_of(hot_accum, hot_sum)
    for j in (1, 3, 2):
        a = (p1 + 4 - j) % 4
        landed(g.at[p2, a], s1.at[j], r1.at[j])
        for d in (1, 3, 2):
            forward(d, j, (0, 4))
        select(p2, a, (0, j))
        add_hot(p2, a)

    def pass_on(d, j):
        select((p2 + 4 - d) % 4, (p1 + 4 - j) % 4, (d, j))
        if d == 2:
            send_scales(j)

    for j in (1, 3, 2):
        for d in (1, 3, 2):
            forward(d, j, (1, 2, 3))
    for d in (1, 3, 2):
        b = (p2 + 4 - d) % 4
        landed(g.at[b, p1], s2.at[d, 0], r2.at[d, 0])
        add_hot(b, p1)
        pass_on(d, 0)
    for j in (1, 3, 2):
        for d in (1, 3, 2):
            arrives(d, j, (0, 4))
            add_hot((p2 + 4 - d) % 4, (p1 + 4 - j) % 4)
    send(hp.at[twin_part], hr, s5.at[0], r5.at[0], twin)
    landed(hr, s5.at[0], r5.at[0])
    hs[...] = hp[part] + hr[...]
    for m in (2, 6, 4):
        send(hs, hz.at[m // 2], s6.at[m // 2], r6.at[m // 2], along_z(m)[1])
    for j in (1, 3, 2):
        for d in (1, 3, 2):
            arrives(d, j, (1, 2, 3))
            pass_on(d, j)

    for m in (1, 3, 2):
        landed(hz.at[m], s6.at[m], r6.at[m])
    hot_grad[x, y, part] = hs[...] + hz[1] + hz[2] + hz[3]
    piece = hot_grad.at[x, y, part]
    for d in (1, 3, 2):
        send(piece, piece, s7.at[d], r7.at[d], plane((p1 + d) % 4, p2))
    for d in (1, 3, 2):
        send(piece, piece, s8.at[d, 0], r8.at[d, 0], plane(p1, (p2 + d) % 4))
    send(piece, piece, s9.at[0, 0], r9.at[0, 0], twin)
    steps = 4096 // ROW_STEP
    scatter(chunk(0), 0, steps, first=True)
    for j in (1, 3, 2):
        xx, yy = share((p1 + 4 - j) % 4, p2)
        piece = hot_grad.at[xx, yy, part]
        landed(piece, s7.at[j], r7.at[j])
        for d in (1, 3, 2):
            send(piece, piece, s8.at[d, j], r8.at[d, j], plane(p1, (p2 + d) % 4))
        send(piece, piece, s9.at[0, j], r9.at[0, j], twin)
    scatter(chunk(1), 0, steps)
    scatter(chunk(3), 0, steps)
    for j in (0, 1, 3, 2):
        for d in (1, 3, 2):
            xx, yy = share((p1 + 4 - j) % 4, (p2 + 4 - d) % 4)
            piece = hot_grad.at[xx, yy, part]
            landed(piece, s8.at[d, j], r8.at[d, j])
            send(piece, piece, s9.at[d, j], r9.at[d, j], twin)
    scatter(chunk(2), 0, steps, last=True)
    rows_of(cold_sum, cold_accum_new)
    for j in (0, 1, 3, 2):
        for d in (0, 1, 3, 2):
            q1 = (x + c * (y - x) + 4 - j) % 4
            q2 = (y + c * (x - y) + 4 - d) % 4
            xx = q1 + c * (q2 - q1)
            yy = q2 + c * (q1 - q2)
            landed(hot_grad.at[xx, yy, twin_part], s9.at[d, j], r9.at[d, j])
    for t in range(4):
        fresh, new = adagrad_rows(hot_grad[t].reshape(512, SEL), hot_w[t], hot_sum[t])
        hot_new[t] = fresh
        hot_sum[t] = new
    rows_of(hot_sum, hot_accum_new)
    for copy in sends:
        copy.wait_send()


def step(*args):
    dma = pltpu.SemaphoreType.DMA
    vmem = pl.BlockSpec(memory_space=pltpu.VMEM)
    hbm = pl.BlockSpec(memory_space=pltpu.HBM)
    outs = args[5:]
    args = [pltpu.with_memory_space_constraint(a, pltpu.HBM) for a in args]
    return pl.pallas_call(
        step_kernel,
        out_shape=tuple(jax.ShapeDtypeStruct(a.shape, F32) for a in outs),
        in_specs=[hbm] * 9,
        out_specs=(vmem,) * 4,
        scratch_shapes=[
            pltpu.VMEM((4, 4, BLOCK_ROWS, SEL), BF16),
            pltpu.VMEM((8, 4, 4, 32, SEL), BF16),
            pltpu.VMEM((4, 8, 1, 128), F32),
            pltpu.VMEM((8, 4, 4, 32, SEL), BF16),
            pltpu.VMEM((8, 4, 1, 128), F32),
            pltpu.VMEM((8, 16, SEL), F32),
            pltpu.VMEM((4, 16, SEL), F32),
            pltpu.VMEM((4, 16, SEL), F32),
            pltpu.VMEM((4, 4, 16, SEL), F32),
            pltpu.VMEM((4, 4, 8, 16, SEL), F32),
            pltpu.VMEM((128, 128), F32),
            pltpu.VMEM((128, 128), F32),
            pltpu.VMEM(outs[0].shape, F32),
            pltpu.VMEM(outs[2].shape, F32),
            pltpu.VMEM((*outs[0].shape[:2], 128), F32),
            pltpu.VMEM((*outs[2].shape[:2], 128), F32),
            *(pltpu.VMEM(a.shape, a.dtype) for a in (*args[:5], args[6], args[8])),
            dma((9,)),
            dma((4,)), dma((4,)),
            dma((4, 4)), dma((4, 4)),
            dma((8, 16)), dma((8, 16)),
            dma((8, 4)), dma((8, 4)),
            dma((1,)), dma((1,)),
            dma((4,)), dma((4,)),
            dma((4,)), dma((4,)),
            dma((4, 4)), dma((4, 4)),
            dma((4, 4)), dma((4, 4)),
            dma((4, 4, 5)), dma((4, 4, 5)),
        ],
        compiler_params=pltpu.CompilerParams(
            collective_id=0, has_side_effects=True, vmem_limit_bytes=40 * 1024 * 1024
        ),
        name="step",
    )(*args)


def leave_kernel(*refs):
    sem = refs[-1]
    copies = [
        pltpu.make_async_copy(refs[n], refs[4 + n], sem.at[n]) for n in range(4)
    ]
    for copy in copies:
        copy.start()
    for copy in copies:
        copy.wait()


def leave(*arrays):
    return pl.pallas_call(
        leave_kernel,
        out_shape=tuple(jax.ShapeDtypeStruct(a.shape, a.dtype) for a in arrays),
        in_specs=[pl.BlockSpec(memory_space=pltpu.VMEM)] * 4,
        out_specs=(pl.BlockSpec(memory_space=pl.ANY),) * 4,
        scratch_shapes=[pltpu.SemaphoreType.DMA((4,))],
        compiler_params=pltpu.CompilerParams(vmem_limit_bytes=16 * 1024 * 1024),
        name="leave",
    )(*arrays)


def per_device(
    pooled_grad,
    grad_scale,
    hot_slot,
    send_index,
    recv_row,
    cold_weight,
    cold_accum,
    hot_weight,
    hot_accum,
):
    results = step(
        pooled_grad,
        send_index[0].T,
        grad_scale.T,
        hot_slot.transpose(1, 2, 0),
        recv_row[0].T,
        cold_weight,
        cold_accum,
        hot_weight,
        hot_accum,
    )
    return leave(*results)


def solution(mesh):
    in_specs = (
        P(NODE_CHIP, None, None),
        P(NODE_CHIP, None),
        P(NODE_CHIP, None, None),
        P(NODE_CHIP, None, None),
        P(NODE_CHIP, None, None),
        P(None, NODE_CHIP, None),
        P(None, NODE_CHIP),
        P(),
        P(),
    )
    out_specs = (P(None, NODE_CHIP, None), P(None, NODE_CHIP), P(), P())
    return jax.shard_map(
        per_device, mesh=mesh, in_specs=in_specs, out_specs=out_specs, check_vma=False
    )
```
